32 devices in a mesh: row: 4 (over y, core), col: 8 (over z, x).
Axes of the slice: x: 2, y: 2, z: 4, core: 2. Of those that a mesh axis runs over, the one named last changes fastest.
Arguments:
- start_field: float32 [1, 2, 4096, 8192], P(None, None, 'col', 'row'), may hold values from -6 to 6
- section_field: float32 [1, 2, 4096, 8192], P(None, None, 'col', 'row'), may hold values from -26 to 26
- start_term: float32 [1, 2, 4096, 8192], P(None, None, 'col', 'row'), may hold values from -6 to 6
- first_term: float32 [1, 2, 4096, 8192], P(None, None, 'col', 'row'), may hold values from -6 to 6
- second_term: float32 [1, 2, 4096, 8192], P(None, None, 'col', 'row'), may hold values from -6 to 6
Outputs:
- next_field: float32 [1, 2, 4096, 8192], P(None, None, 'col', 'row')
The draws below stay inside these ranges and needn't reach their ends.
All inputs are finite; a program needn't handle non-finite values.
Results may differ from the reference program's by a relative error of at most 0.0001.
Values sent between devices are 32-bit elements; how exact they have to be, the bound alone decides.
A program may use at most 256 MiB of HBM per device.

```python
import math
import jax
import jax.numpy as jnp
from jax import lax

N = 8192
MEMBERS = 1
NK = 4096


def draw_section_field(key, part):
    wave_x = lax.broadcasted_iota(jnp.int32, (NK, N), 0)
    index_y = lax.broadcasted_iota(jnp.int32, (NK, N), 1)
    wave_y = jnp.where(index_y < N // 2, index_y, index_y - N)
    envelope = 3.0 * jnp.sqrt((wave_x * wave_x + wave_y * wave_y).astype(jnp.float32)) / N
    noise = jnp.clip(jax.random.normal(key, (MEMBERS, 2, NK, N), jnp.float32), -6.0, 6.0)
    return 2.0 * envelope * noise


def steps_of(key, dims, split, smallest, largest):
    factor_of, own = 1.0, jax.random.fold_in(key, 6)
    for dim, blocks in split:
        steps = jnp.exp(jax.random.uniform(jax.random.fold_in(own, dim), (blocks,), jnp.float32, smallest / len(split), largest / len(split)))
        factor_of = factor_of * jnp.repeat(steps, dims[dim] // blocks).reshape([-1 if axis == dim else 1 for axis in range(len(dims))])
    return factor_of


def gaussian(key, extent, deviation, limit, cuts=(), dtype=jnp.bfloat16):
    drawn = deviation * jax.random.normal(key, extent, jnp.float32)
    if cuts:
        drawn = drawn * steps_of(key, extent, cuts, -0.22, 0.18)
    return jnp.clip(drawn, -limit, limit).astype(dtype)


def setup_inputs(seed: int = 0) -> dict:
    seeds = jax.random.split(jax.random.key(seed), 6)
    start_field = gaussian(seeds[0], (MEMBERS, 2, NK, N), 1.0, 6.0, ((2, 8), (3, 4)), jnp.float32)
    section_field = draw_section_field(jax.random.fold_in(seeds[5], 71), 0)
    start_term = gaussian(seeds[2], (MEMBERS, 2, NK, N), 1.0, 6.0, ((2, 8), (3, 4)), jnp.float32)
    first_term = gaussian(seeds[3], (MEMBERS, 2, NK, N), 1.0, 6.0, ((2, 8), (3, 4)), jnp.float32)
    second_term = gaussian(seeds[4], (MEMBERS, 2, NK, N), 1.0, 6.0, ((2, 8), (3, 4)), jnp.float32)
    return dict(start_field=start_field, section_field=section_field, start_term=start_term, first_term=first_term, second_term=second_term)


viscous_rate = 1.5
wave_scale = 3.0
series_terms = 12


def section_weights(wave_x, wave_y, length):
    square = wave_x * wave_x + wave_y * wave_y
    kappa_x = wave_scale * wave_x.astype(jnp.float32) / length
    kappa_y = wave_scale * wave_y.astype(jnp.float32) / length
    kappa_sq = kappa_x * kappa_x + kappa_y * kappa_y
    zvalue = -viscous_rate * kappa_sq
    damping = jnp.exp(zvalue)
    near_zero = 27 * square < 2 * length * length

    def series(degree):
        running = jnp.full_like(zvalue, 1.0 / math.factorial(series_terms - 1 + degree))
        for term_index in range(series_terms - 2, -1, -1):
            running = running * zvalue + 1.0 / math.factorial(term_index + degree)
        return running

    clamped = jnp.where(near_zero, -1.0, zvalue)
    exp_clamped = jnp.exp(clamped)
    closed_one = (exp_clamped - 1.0) / clamped
    closed_two = (exp_clamped - 1.0 - clamped) / (clamped * clamped)
    closed_three = (exp_clamped - 1.0 - clamped - 0.5 * clamped * clamped) / (clamped * clamped * clamped)
    phi_one = jnp.where(near_zero, series(1), closed_one)
    phi_two = jnp.where(near_zero, series(2), closed_two)
    phi_three = jnp.where(near_zero, series(3), closed_three)
    weight_a = phi_one - 3.0 * phi_two + 4.0 * phi_three
    weight_b = phi_two - 2.0 * phi_three
    weight_c = 4.0 * phi_three - phi_two
    keep_mask = ((3 * jnp.abs(wave_x) < length) & (3 * jnp.abs(wave_y) < length)).astype(jnp.float32)
    inverse_sq = (length * length) / (9.0 * jnp.maximum(square, 1).astype(jnp.float32))
    return damping, weight_a, weight_b, weight_c, kappa_x, kappa_y, keep_mask, inverse_sq


def to_grid(real_part, imag_part):
    length = real_part.shape[1]
    complex_spec = lax.complex(real_part, imag_part)
    along_y = jnp.fft.ifft(complex_spec, axis=1)
    return jnp.fft.irfft(along_y, n=length, axis=0) * length


def to_spectrum(real_grid):
    length = real_grid.shape[0]
    along_x = jnp.fft.rfft(real_grid, axis=0)[: length // 2]
    spectrum = jnp.fft.fft(along_x, axis=1) / length
    return jnp.real(spectrum), jnp.imag(spectrum)


def reference(start_field, section_field, start_term, first_term, second_term):
    length = start_field.shape[3]
    wave_x = lax.broadcasted_iota(jnp.int32, (length // 2, length), 0)
    index_y = lax.broadcasted_iota(jnp.int32, (length // 2, length), 1)
    wave_y = jnp.where(index_y < length // 2, index_y, index_y - length)
    damping, weight_a, weight_b, weight_c, kappa_x, kappa_y, keep_mask, inverse_sq = section_weights(wave_x, wave_y, length)
    section_terms = []
    for member in range(section_field.shape[0]):
        real_part = section_field[member, 0] * keep_mask
        imag_part = section_field[member, 1] * keep_mask
        psi_real = real_part * inverse_sq
        psi_imag = imag_part * inverse_sq
        vel_u = to_grid(-kappa_y * psi_imag, kappa_y * psi_real)
        grad_x = to_grid(-kappa_x * imag_part, kappa_x * real_part)
        jacobian = vel_u * grad_x
        vel_v = to_grid(kappa_x * psi_imag, -kappa_x * psi_real)
        grad_y = to_grid(-kappa_y * imag_part, kappa_y * real_part)
        jacobian = jacobian + vel_v * grad_y
        jac_real, jac_imag = to_spectrum(jacobian)
        section_terms.append(jnp.stack([-keep_mask * jac_real, -keep_mask * jac_imag]))
    section_term = jnp.stack(section_terms)
    return damping * start_field + weight_a * start_term + 2.0 * weight_b * (first_term + second_term) + weight_c * section_term
```

```python
import functools
import math

import jax
import jax.numpy as jnp
from jax import lax
from jax.experimental import pallas as pl
from jax.experimental.pallas import tpu as pltpu
from jax.sharding import PartitionSpec as P

RADIX = 128


viscous_rate = 1.5
wave_scale = 3.0
series_terms = 12


def section_weights(wave_x, wave_y, length):
    square = wave_x * wave_x + wave_y * wave_y
    kappa_x = wave_scale * wave_x.astype(jnp.float32) / length
    kappa_y = wave_scale * wave_y.astype(jnp.float32) / length
    kappa_sq = kappa_x * kappa_x + kappa_y * kappa_y
    zvalue = -viscous_rate * kappa_sq
    damping = jnp.exp(zvalue)
    near_zero = 27 * square < 2 * length * length

    def series(degree):
        running = jnp.full_like(zvalue, 1.0 / math.factorial(series_terms - 1 + degree))
        for term_index in range(series_terms - 2, -1, -1):
            running = running * zvalue + 1.0 / math.factorial(term_index + degree)
        return running

    clamped = jnp.where(near_zero, -1.0, zvalue)
    exp_clamped = jnp.exp(clamped)
    closed_one = (exp_clamped - 1.0) / clamped
    closed_two = (exp_clamped - 1.0 - clamped) / (clamped * clamped)
    closed_three = (exp_clamped - 1.0 - clamped - 0.5 * clamped * clamped) / (
        clamped * clamped * clamped
    )
    phi_one = jnp.where(near_zero, series(1), closed_one)
    phi_two = jnp.where(near_zero, series(2), closed_two)
    phi_three = jnp.where(near_zero, series(3), closed_three)
    weight_a = phi_one - 3.0 * phi_two + 4.0 * phi_three
    weight_b = phi_two - 2.0 * phi_three
    weight_c = 4.0 * phi_three - phi_two
    keep_mask = ((3 * jnp.abs(wave_x) < length) & (3 * jnp.abs(wave_y) < length)).astype(
        jnp.float32
    )
    inverse_sq = length * length / (9.0 * jnp.maximum(square, 1).astype(jnp.float32))
    return (damping, weight_a, weight_b, weight_c, kappa_x, kappa_y, keep_mask, inverse_sq)


def section_table(count_in, count_out, period, direction):
    row_ids = lax.broadcasted_iota(jnp.int32, (count_in, count_out), 0)
    col_ids = lax.broadcasted_iota(jnp.int32, (count_in, count_out), 1)
    angles = direction * 2.0 * math.pi / period * (row_ids * col_ids % period).astype(jnp.float32)
    cosine = jnp.cos(angles)
    sine_part = jnp.sin(angles)
    return jnp.stack(
        [jnp.stack([cosine, sine_part], axis=1), jnp.stack([-sine_part, cosine], axis=1)], axis=0
    )


def twiddle(count_c, count_b, period, direction):
    row_ids = lax.broadcasted_iota(jnp.int32, (count_c, count_b), 0)
    col_ids = lax.broadcasted_iota(jnp.int32, (count_c, count_b), 1)
    angles = direction * 2.0 * math.pi / period * (row_ids * col_ids % period).astype(jnp.float32)
    return (jnp.cos(angles), jnp.sin(angles))


def rotate(values, cosine, sine_part):
    return jnp.stack(
        [values[0] * cosine - values[1] * sine_part, values[0] * sine_part + values[1] * cosine]
    )


def product(equation, left, right):
    return jnp.einsum(equation, left, right, precision=lax.Precision.HIGH)


def lines_inverse(pieces):
    parts, count_k, length = pieces.shape
    count_b = RADIX
    count_a = length // count_b
    shaped = pieces.reshape((parts, count_k, count_a, count_b))
    first = product("pkab,pasc->skcb", shaped, section_table(count_a, count_a, count_a, 1.0))
    first = rotate(first, *twiddle(count_a, count_b, length, 1.0))
    second = product("pkcb,pbsd->skcd", first, section_table(count_b, count_b, count_b, 1.0))
    return second.reshape((parts, count_k, length))


def lines_forward(pieces):
    parts, count_k, length = pieces.shape
    count_d = RADIX
    count_c = length // count_d
    shaped = pieces.reshape((parts, count_k, count_c, count_d))
    first = product("pkcd,pdsf->skcf", shaped, section_table(count_d, count_d, count_d, -1.0))
    first = rotate(first, *twiddle(count_c, count_d, length, -1.0))
    second = product("pkcf,pcse->skef", first, section_table(count_c, count_c, count_c, -1.0))
    return second.reshape((parts, count_k, length))


def turned_table(count_c, count_b, period, direction):
    c_ids = lax.broadcasted_iota(jnp.int32, (count_c, count_b, count_b), 0)
    b_ids = lax.broadcasted_iota(jnp.int32, (count_c, count_b, count_b), 1)
    d_ids = lax.broadcasted_iota(jnp.int32, (count_c, count_b, count_b), 2)
    steps = b_ids * (c_ids + count_c * d_ids) % period
    angles = direction * 2.0 * math.pi / period * steps.astype(jnp.float32)
    return jnp.cos(angles), jnp.sin(angles)


def columns_inverse(pieces, table):
    parts, half_count, count_y = pieces.shape
    count_a = half_count // RADIX
    count_c = 2 * count_a
    shaped = pieces.reshape((parts, count_a, RADIX, count_y))
    first = product("paby,pasc->csby", shaped, section_table(count_a, count_c, count_c, 1.0))
    return product("csby,csbd->cdy", first, table)


def columns_forward(grid, table):
    count_c, count_d, count_y = grid.shape
    half_count = count_c // 2
    first = product("cdy,cpfd->cpfy", grid, table)
    second = product(
        "cpfy,pcse->sefy", first, section_table(count_c, half_count, count_c, -1.0)
    )
    return second.reshape((2, half_count * count_d, count_y))


def to_columns(lines):
    return lax.all_to_all(lines, ("col", "row"), split_axis=2, concat_axis=1, tiled=True)


def to_lines(columns):
    return lax.all_to_all(columns, ("col", "row"), split_axis=1, concat_axis=2, tiled=True)


def positions(shape, start_x, start_y, length):
    wave_x = start_x + lax.broadcasted_iota(jnp.int32, shape, 0)
    index_y = start_y + lax.broadcasted_iota(jnp.int32, shape, 1)
    wave_y = jnp.where(index_y < length // 2, index_y, index_y - length)
    return wave_x, wave_y


def nonlinear(section_field, length):
    block_x = section_field.shape[1]
    lines = lax.all_to_all(section_field, "row", split_axis=1, concat_axis=2, tiled=True)
    count_k = lines.shape[1]
    start_x = lax.axis_index("col") * block_x + lax.axis_index("row") * count_k
    wave_x, wave_y = positions((count_k, length), start_x, 0, length)
    square = wave_x * wave_x + wave_y * wave_y
    kappa_x = wave_scale * wave_x.astype(jnp.float32) / length
    kappa_y = wave_scale * wave_y.astype(jnp.float32) / length
    keep = (3 * jnp.abs(wave_x) < length) & (3 * jnp.abs(wave_y) < length)
    doubled = jnp.where(wave_x == 0, 1.0, 2.0) * (1.0 / length)
    inverse_sq = length * length / (9.0 * jnp.maximum(square, 1).astype(jnp.float32))
    factor = jnp.where(keep, inverse_sq * doubled, 0.0)
    scale_u = kappa_y * factor
    scale_v = kappa_x * factor
    spec_u = jnp.stack([-scale_u * lines[1], scale_u * lines[0]])
    spec_v = jnp.stack([scale_v * lines[1], -scale_v * lines[0]])
    count_c = length // RADIX
    cosine, sine_part = turned_table(count_c, RADIX, length, 1.0)
    table = jnp.stack([cosine, -sine_part], axis=1)
    vel_u = columns_inverse(to_columns(lines_inverse(spec_u)), table)
    vel_v = columns_inverse(to_columns(lines_inverse(spec_v)), table)
    cross = lines_forward(to_lines(columns_forward(vel_u * vel_v, table)))
    square_gap = lines_forward(
        to_lines(columns_forward((vel_v - vel_u) * (vel_v + vel_u), table))
    )
    scale = jnp.where(keep, 1.0 / length, 0.0)
    weight_cross = (kappa_x * kappa_x - kappa_y * kappa_y) * scale
    weight_gap = kappa_x * kappa_y * scale
    term = weight_cross * cross + weight_gap * square_gap
    return lax.all_to_all(term, "row", split_axis=2, concat_axis=1, tiled=True)


def per_device(start_field, section_field, start_term, first_term, second_term):
    members = start_field.shape[0]
    block_x = start_field.shape[2]
    block_y = start_field.shape[3]
    length = block_y * lax.axis_size("row")
    wave_x, wave_y = positions(
        (block_x, block_y),
        lax.axis_index("col") * block_x,
        lax.axis_index("row") * block_y,
        length,
    )
    damping, weight_a, weight_b, weight_c = section_weights(wave_x, wave_y, length)[:4]
    linear = (
        damping * start_field
        + weight_a * start_term
        + 2.0 * weight_b * (first_term + second_term)
    )
    linear, weight_c = lax.optimization_barrier((linear, weight_c))
    section_term = jnp.stack([nonlinear(section_field[m], length) for m in range(members)])
    return linear + weight_c * section_term


LANES = 128
SUBL = 8
HALF = 64


def plan_of(length, rows, cols, block_x, block_y):
    if length != LANES * HALF or rows != 4 or block_x % (rows * SUBL) or block_y * rows != length:
        return None
    kept = (length - 1) // 3 + 1
    stride = rows * SUBL
    groups = block_x // stride
    own = [min(groups, max(0, -(-(kept - c * block_x) // stride))) for c in range(cols)]
    slots = -(-sum(own) // cols)
    extra = groups - slots
    donors = [c for c in range(cols) if own[c] == groups]
    if extra <= 0 or 2 * extra > slots or any(slots < own[c] < groups for c in range(cols)):
        return None
    takers = [c for c in range(cols) if own[c] + extra <= slots]
    first = [(c, 0) for c in takers]
    second = [(c, 1) for c in takers if own[c] == 0]
    places = first + second
    if len(donors) > len(places):
        return None
    order = donors[-1:] + donors[:-1]
    moves = [(donor, taker, turn) for donor, (taker, turn) in zip(order, places)]
    low = (kept + LANES - 1) // LANES
    high = HALF - (length - kept + 1) // LANES
    if low != high or low % 2 or low > HALF // 2:
        return None
    per = low // 2
    home_tiles = block_y // LANES
    if not per < home_tiles < low:
        return None
    return dict(
        kept=kept, stride=stride, groups=groups, own=own, slots=slots, extra=extra,
        moves=moves, low=low, per=per, home=home_tiles, rows=rows, cols=cols,
        block_x=block_x, block_y=block_y, length=length,
    )


def home_of(plan, group):
    per_block = plan["block_x"] // SUBL
    if group * SUBL >= plan["kept"]:
        return None
    col, inside = divmod(group, per_block)
    slot = inside // plan["rows"]
    if slot < plan["slots"]:
        return col, slot
    for donor, taker, turn in plan["moves"]:
        if donor == col:
            start = plan["slots"] - plan["extra"] if turn == 0 else 0
            return taker, start + slot - plan["slots"]
    raise ValueError("no place")


def line_info(plan):
    rows = []
    slots, extra = plan["slots"], plan["extra"]
    for col in range(plan["cols"]):
        base = [col * plan["block_x"] + slot * plan["stride"] for slot in range(slots)]
        flags = [0, 0]
        for donor, taker, turn in plan["moves"]:
            if taker == col:
                flags[turn] = 1
                start = slots - extra if turn == 0 else 0
                for step in range(extra):
                    base[start + step] = donor * plan["block_x"] + (slots + step) * plan["stride"]
        rows.append(base + flags)
    return rows


def cadd(a, b):
    if a is None:
        return b
    if b is None:
        return a
    return (a[0] + b[0], a[1] + b[1])


def csub(a, b):
    if b is None:
        return a
    if a is None:
        return (-b[0], -b[1])
    return (a[0] - b[0], a[1] - b[1])


def cturn(a, step, period, sign):
    if a is None:
        return None
    step = step * sign % period
    if step == 0:
        return a
    if 4 * step == period:
        return (-a[1], a[0])
    if 2 * step == period:
        return (-a[0], -a[1])
    if 4 * step == 3 * period:
        return (a[1], -a[0])
    angle = 2.0 * math.pi * step / period
    cosine, sine_part = math.cos(angle), math.sin(angle)
    if 8 * step % period == 0:
        size = math.sqrt(0.5)
        sign_c, sign_s = (1 if cosine > 0 else -1), (1 if sine_part > 0 else -1)
        real = a[0] - a[1] if sign_c == sign_s else a[0] + a[1]
        imag = a[0] + a[1] if sign_c == sign_s else a[1] - a[0]
        return (real * (sign_c * size), imag * (sign_c * size))
    return (a[0] * cosine - a[1] * sine_part, a[0] * sine_part + a[1] * cosine)


def butterflies(values, sign, need):
    count = len(values)
    if all(v is None for v in values):
        return {k: None for k in need}
    if count == 1:
        return {k: values[0] for k in need}
    half = count // 2
    sub = sorted({k % half for k in need})
    even = butterflies(values[0::2], sign, sub)
    odd = butterflies(values[1::2], sign, sub)
    wanted = set(need)
    out = {}
    for k in sub:
        turned = cturn(odd[k], k, count, sign)
        if k in wanted:
            out[k] = cadd(even[k], turned)
        if k + half in wanted:
            out[k + half] = csub(even[k], turned)
    return out


def halves(values):
    high = values.astype(jnp.bfloat16)
    return high, (values - high.astype(jnp.float32)).astype(jnp.bfloat16)


def dot3(left, right):
    lh, ll = left
    rh, rl = right
    def mm(a, b):
        return jnp.dot(a, b, preferred_element_type=jnp.float32)
    return mm(lh, rh) + (mm(ll, rh) + mm(lh, rl))


def tile_of(plan, a):
    low = plan["low"]
    t = a if a < low else a - (HALF - 2 * low)
    return t // plan["per"], (t % plan["per"]) * LANES


def kept_tiles(plan):
    low = plan["low"]
    return list(range(low)) + list(range(HALF - low, HALF))


def sublane_iota():
    return lax.broadcasted_iota(jnp.int32, (SUBL, LANES), 0)


def lane_iota():
    return lax.broadcasted_iota(jnp.int32, (SUBL, LANES), 1)


def keep_of(plan, wave_x, wave_y):
    return (3 * wave_x < plan["length"]) & (3 * jnp.abs(wave_y) < plan["length"])


def lines_in_kernel(plan, parity, info, own, mv1, mv2, turn, wh, wl, out, scr):
    slots, extra, length = plan["slots"], plan["extra"], plan["length"]
    j = pl.program_id(0)
    use1 = (info[slots] == 1) & (j >= slots - extra)
    use2 = (info[slots + 1] == 1) & (j < extra)
    wave_x = info[j] + sublane_iota()
    kx = wave_x.astype(jnp.float32)
    doubled = jnp.where(wave_x == 0, 1.0, 2.0) * (length / 9.0)
    step = wave_scale / length
    lane = lane_iota()
    for field in range(2):
        tiles = {}
        for a in kept_tiles(plan):
            r, off = tile_of(plan, a)
            wave_y = lane + (LANES * a - (length if a >= HALF // 2 else 0))
            square = (wave_x * wave_x + wave_y * wave_y)
            value = doubled / jnp.maximum(square, 1).astype(jnp.float32)
            factor = jnp.where(keep_of(plan, wave_x, wave_y), value, 0.0)
            if field == 0:
                factor = factor * (step * wave_y.astype(jnp.float32))
            else:
                factor = factor * (-step * kx)
            parts = []
            for p in range(2):
                at = (r, p, slice(None), slice(off, off + LANES))
                parts.append(jnp.where(use1, mv1[at], jnp.where(use2, mv2[at], own[at])))
            tiles[a] = (-factor * parts[1], factor * parts[0])
        mixed = []
        for a in range(HALF // 2):
            x0, x1 = tiles.get(a), tiles.get(a + HALF // 2)
            if parity == 0:
                mixed.append(cadd(x0, x1))
            else:
                mixed.append(cturn(csub(x0, x1), a, HALF, 1))
        result = butterflies(mixed, 1, range(HALF // 2))
        for e in range(HALF // 2):
            re, im = result[e]
            cosine, sine_part = turn[e, 0:1, :], turn[e, 1:2, :]
            at = slice(SUBL * e, SUBL * (e + 1))
            scr[at, 0:LANES] = re * cosine - im * sine_part
            scr[at, LANES:] = re * sine_part + im * cosine
        spread = dot3(halves(scr[...]), (wh[...], wl[...]))
        for s in range(2):
            out[:, field, s] = spread[:, s * LANES:(s + 1) * LANES].reshape(
                HALF // 2, SUBL, LANES
            )


def lines_in(plan, parity, info, own, mv1, mv2, turn, table):
    slots, extra, rows = plan["slots"], plan["extra"], plan["rows"]
    width = plan["per"] * LANES
    block = (rows, 2, SUBL, width)
    devices = rows * plan["cols"]
    whole = lambda shape: pl.BlockSpec(shape, lambda j: (0,) * len(shape))
    return pl.pallas_call(
        functools.partial(lines_in_kernel, plan, parity),
        grid=(slots,),
        in_specs=[
            pl.BlockSpec(memory_space=pltpu.SMEM),
            pl.BlockSpec(block, lambda j: (0, 0, j, 0)),
            pl.BlockSpec(block, lambda j: (0, 0, jnp.maximum(j - (slots - extra), 0), 0)),
            pl.BlockSpec(block, lambda j: (0, 0, jnp.minimum(j, extra - 1), 0)),
            whole((HALF // 2, 2, LANES)),
            whole((2 * LANES, 2 * LANES)),
            whole((2 * LANES, 2 * LANES)),
        ],
        out_specs=pl.BlockSpec((devices, 2, 2, SUBL, LANES), lambda j: (0, 0, 0, j, 0)),
        out_shape=jax.ShapeDtypeStruct((devices, 2, 2, slots * SUBL, LANES), jnp.float32),
        scratch_shapes=[pltpu.VMEM((HALF // 2 * SUBL, 2 * LANES), jnp.float32)],
        compiler_params=pltpu.CompilerParams(vmem_limit_bytes=50 << 20),
        cost_estimate=pl.CostEstimate(flops=4 << 30, bytes_accessed=16 << 20, transcendentals=0),
        name="lines_in",
    )(info, own, mv1, mv2, turn, *table)


def columns_kernel(plan, src, th, tl, fh, fl, out, mid):
    rows = plan["rows"]
    low = plan["low"]
    per_tile = LANES // SUBL
    quarter = per_tile // rows
    inside = [[home_of(plan, a * per_tile + q * rows) for a in range(low)] for q in range(quarter)]
    used = {place for line in inside for place in line if place}

    @pl.loop(0, 2 * rows)
    def _(i):
        r = i % rows
        field = i // rows
        lanes = pl.ds(pl.multiple_of(field * LANES, LANES), LANES)
        for q in range(quarter):
            values = []
            for a in range(HALF):
                place = inside[q][a] if a < low else None
                if place is None:
                    values.append(None)
                    continue
                at = pl.ds(place[1] * SUBL, SUBL)
                dev = place[0] * rows + r
                values.append((src[dev, field, 0, at, :], src[dev, field, 1, at, :]))
            result = butterflies(values, 1, range(HALF))
            base = pl.multiple_of((q * rows + r) * SUBL, SUBL)
            for c in range(HALF):
                mid[c, pl.ds(base, SUBL), lanes] = result[c][0]
                mid[c, pl.ds(LANES + base, SUBL), lanes] = result[c][1]

    @pl.loop(0, HALF)
    def _(c):
        grid = dot3((th[c], tl[c]), halves(mid[c]))
        u, v = grid[:, :LANES], grid[:, LANES:]
        pair = jnp.concatenate([u * v, (v - u) * (v + u)], axis=1)
        mid[c] = dot3((fh[c], fl[c]), halves(pair))

    @pl.loop(0, 2 * rows)
    def _(i):
        r = i % rows
        field = i // rows
        lanes = pl.ds(pl.multiple_of(field * LANES, LANES), LANES)
        for q in range(quarter):
            base = pl.multiple_of((q * rows + r) * SUBL, SUBL)
            values = [
                (mid[c, pl.ds(base, SUBL), lanes], mid[c, pl.ds(LANES + base, SUBL), lanes])
                for c in range(HALF)
            ]
            need = [a for a in range(low) if inside[q][a]]
            result = butterflies(values, -1, need)
            for a in need:
                place = inside[q][a]
                at = pl.ds(place[1] * SUBL, SUBL)
                dev = place[0] * rows + r
                out[dev, field, 0, at, :] = result[a][0]
                out[dev, field, 1, at, :] = result[a][1]
        for col in range(plan["cols"]):
            for slot in range(plan["slots"]):
                if (col, slot) not in used:
                    for p in range(2):
                        out[col * rows + r, field, p, pl.ds(slot * SUBL, SUBL), :] = jnp.zeros(
                            (SUBL, LANES), jnp.float32
                        )


def columns(plan, spread, tables):
    return pl.pallas_call(
        functools.partial(columns_kernel, plan),
        in_specs=[pl.BlockSpec(memory_space=pltpu.VMEM)] * 5,
        out_specs=pl.BlockSpec(memory_space=pltpu.VMEM),
        out_shape=jax.ShapeDtypeStruct(spread.shape, jnp.float32),
        scratch_shapes=[pltpu.VMEM((HALF, 2 * LANES, 2 * LANES), jnp.float32)],
        compiler_params=pltpu.CompilerParams(vmem_limit_bytes=60 << 20),
        cost_estimate=pl.CostEstimate(flops=16 << 30, bytes_accessed=30 << 20, transcendentals=0),
        name="columns",
    )(spread, *tables)


def lines_out_kernel(plan, info, got0, got1, turn, wh, wl, own, mv1, mv2, scr, acc):
    slots, extra, length = plan["slots"], plan["extra"], plan["length"]
    j = pl.program_id(0)
    wave_x = info[j] + sublane_iota()
    step = wave_scale / length
    kappa_x = step * wave_x.astype(jnp.float32)
    lane = lane_iota()
    tiles = kept_tiles(plan)
    rows = HALF // 2 * SUBL
    for field in range(2):
        for parity, got in enumerate((got0, got1)):
            both = jnp.concatenate(
                [got[:, field, s].reshape(rows, LANES) for s in range(2)], axis=1
            )
            scr[parity] = dot3(halves(both), (wh[...], wl[...]))
        values = []
        for c in range(HALF):
            e, parity = c // 2, c % 2
            at = slice(SUBL * e, SUBL * (e + 1))
            re, im = scr[parity, at, 0:LANES], scr[parity, at, LANES:]
            cosine, sine_part = turn[parity, e, 0:1, :], turn[parity, e, 1:2, :]
            values.append((re * cosine + im * sine_part, im * cosine - re * sine_part))
        result = butterflies(values, -1, tiles)
        for t, a in enumerate(tiles):
            wave_y = lane + (LANES * a - (length if a >= HALF // 2 else 0))
            kappa_y = step * wave_y.astype(jnp.float32)
            keep = keep_of(plan, wave_x, wave_y)
            if field == 0:
                weight = (kappa_x * kappa_x - kappa_y * kappa_y) * (1.0 / length)
            else:
                weight = kappa_x * kappa_y * (1.0 / length)
            r, off = tile_of(plan, a)
            for p in range(2):
                value = jnp.where(keep, weight * result[a][p], 0.0)
                if field == 0:
                    acc[t, p] = value
                else:
                    own[r, p, :, off:off + LANES] = acc[t, p] + value

    @pl.when(j < extra)
    def _():
        mv2[...] = own[...]

    @pl.when(j >= slots - extra)
    def _():
        mv1[...] = own[...]


def lines_out(plan, info, got0, got1, turn, table):
    slots, extra, rows = plan["slots"], plan["extra"], plan["rows"]
    width = plan["per"] * LANES
    block = (rows, 2, SUBL, width)
    devices = rows * plan["cols"]
    whole = lambda shape: pl.BlockSpec(shape, lambda j: (0,) * len(shape))
    got_spec = pl.BlockSpec((devices, 2, 2, SUBL, LANES), lambda j: (0, 0, 0, j, 0))
    lines = lambda n: jax.ShapeDtypeStruct((rows, 2, n * SUBL, width), jnp.float32)
    return pl.pallas_call(
        functools.partial(lines_out_kernel, plan),
        grid=(slots,),
        in_specs=[
            pl.BlockSpec(memory_space=pltpu.SMEM),
            got_spec,
            got_spec,
            whole((2, HALF // 2, 2, LANES)),
            whole((2 * LANES, 2 * LANES)),
            whole((2 * LANES, 2 * LANES)),
        ],
        out_specs=[
            pl.BlockSpec(block, lambda j: (0, 0, j, 0)),
            pl.BlockSpec(block, lambda j: (0, 0, jnp.maximum(j - (slots - extra), 0), 0)),
            pl.BlockSpec(block, lambda j: (0, 0, jnp.minimum(j, extra - 1), 0)),
        ],
        out_shape=[lines(slots), lines(extra), lines(extra)],
        scratch_shapes=[
            pltpu.VMEM((2, HALF // 2 * SUBL, 2 * LANES), jnp.float32),
            pltpu.VMEM((4 * plan["per"], 2, SUBL, LANES), jnp.float32),
        ],
        compiler_params=pltpu.CompilerParams(vmem_limit_bytes=50 << 20),
        cost_estimate=pl.CostEstimate(flops=8 << 30, bytes_accessed=22 << 20, transcendentals=0),
        name="lines_out",
    )(info, got0, got1, turn, *table)


def pack_kernel(plan, info, field, got, own, mv):
    per, home, slots, rows = plan["per"], plan["home"], plan["slots"], plan["rows"]
    j = pl.program_id(0)
    more = home - per
    width, full = per * LANES, home * LANES
    less = width - more * LANES

    def put(dest):
        for p in range(2):
            for r in range(rows):
                at = slice(r * SUBL, (r + 1) * SUBL)

                @pl.when(info[0] == 0)
                def _():
                    dest[r, p] = field[0, p, at, :width]

                @pl.when(info[0] == 1)
                def _():
                    dest[r, p, :, :more * LANES] = got[p, at, :]
                    dest[r, p, :, more * LANES:] = field[0, p, at, :less]

                @pl.when(info[0] == 2)
                def _():
                    dest[r, p, :, :less] = field[0, p, at, full - less:]
                    dest[r, p, :, less:] = got[p, at, :]

                @pl.when(info[0] == 3)
                def _():
                    dest[r, p] = field[0, p, at, full - width:]

    @pl.when(j < slots)
    def _():
        put(own)

    @pl.when(j >= slots)
    def _():
        put(mv)


def pack(plan, where, field, member, got):
    slots, extra, rows, groups = plan["slots"], plan["extra"], plan["rows"], plan["groups"]
    width = plan["per"] * LANES
    more = (plan["home"] - plan["per"]) * LANES
    block = (rows, 2, SUBL, width)
    lines = lambda n: jax.ShapeDtypeStruct((rows, 2, n * SUBL, width), jnp.float32)
    return pl.pallas_call(
        functools.partial(pack_kernel, plan),
        grid=(groups,),
        in_specs=[
            pl.BlockSpec(memory_space=pltpu.SMEM),
            pl.BlockSpec((1, 2, plan["stride"], plan["block_y"]), lambda j: (member, 0, j, 0)),
            pl.BlockSpec((2, plan["stride"], more), lambda j: (0, j, 0)),
        ],
        out_specs=[
            pl.BlockSpec(block, lambda j: (0, 0, jnp.minimum(j, slots - 1), 0)),
            pl.BlockSpec(block, lambda j: (0, 0, jnp.maximum(j - slots, 0), 0)),
        ],
        out_shape=[lines(slots), lines(extra)],
        compiler_params=pltpu.CompilerParams(vmem_limit_bytes=32 << 20),
        cost_estimate=pl.CostEstimate(flops=1 << 24, bytes_accessed=14 << 20, transcendentals=0),
        name="pack",
    )(where, field, got)


def unpack_kernel(plan, info, own, mv, got_own, got_mv, linear, weight, out, term):
    per, home, slots, rows = plan["per"], plan["home"], plan["slots"], plan["rows"]
    j = pl.program_id(0)
    more = (home - per) * LANES
    width, full = per * LANES, home * LANES
    less = width - more
    keep_x = info[1] + j * plan["stride"]

    def put(lines, got):
        for p in range(2):
            for r in range(rows):
                at = slice(r * SUBL, (r + 1) * SUBL)

                @pl.when(info[0] == 0)
                def _():
                    term[p, at, :width] = lines[r, p]
                    term[p, at, width:] = got[r, p]

                @pl.when(info[0] == 1)
                def _():
                    term[p, at, :less] = lines[r, p, :, more:]
                    term[p, at, less:] = jnp.zeros((SUBL, full - less), jnp.float32)

                @pl.when(info[0] == 2)
                def _():
                    term[p, at, full - less:] = lines[r, p, :, :less]
                    term[p, at, :full - less] = jnp.zeros((SUBL, full - less), jnp.float32)

                @pl.when(info[0] == 3)
                def _():
                    term[p, at, full - width:] = lines[r, p]
                    term[p, at, :full - width] = got[r, p]

    @pl.when(j < slots)
    def _():
        put(own, got_own)

    @pl.when(j >= slots)
    def _():
        put(mv, got_mv)

    wave_x = keep_x + lax.broadcasted_iota(jnp.int32, (plan["stride"], full), 0)
    keep = 3 * wave_x < plan["length"]
    for p in range(2):
        out[p] = linear[p] + jnp.where(keep, weight[...] * term[p], 0.0)


def unpack(plan, where, own, mv, got_own, got_mv, linear, weight):
    slots, rows, groups = plan["slots"], plan["rows"], plan["groups"]
    width = plan["per"] * LANES
    more = (plan["home"] - plan["per"]) * LANES
    own_at = lambda j: (0, 0, jnp.minimum(j, slots - 1), 0)
    mv_at = lambda j: (0, 0, jnp.maximum(j - slots, 0), 0)
    rowed = pl.BlockSpec((2, plan["stride"], plan["block_y"]), lambda j: (0, j, 0))
    return pl.pallas_call(
        functools.partial(unpack_kernel, plan),
        grid=(groups,),
        in_specs=[
            pl.BlockSpec(memory_space=pltpu.SMEM),
            pl.BlockSpec((rows, 2, SUBL, width), own_at),
            pl.BlockSpec((rows, 2, SUBL, width), mv_at),
            pl.BlockSpec((rows, 2, SUBL, more), own_at),
            pl.BlockSpec((rows, 2, SUBL, more), mv_at),
            rowed,
            pl.BlockSpec((plan["stride"], plan["block_y"]), lambda j: (j, 0)),
        ],
        out_specs=rowed,
        out_shape=jax.ShapeDtypeStruct(linear.shape, jnp.float32),
        scratch_shapes=[pltpu.VMEM((2, plan["stride"], plan["block_y"]), jnp.float32)],
        compiler_params=pltpu.CompilerParams(vmem_limit_bytes=32 << 20),
        cost_estimate=pl.CostEstimate(flops=1 << 24, bytes_accessed=34 << 20, transcendentals=0),
        name="unpack",
    )(where, own, mv, got_own, got_mv, linear, weight)


def split_table(values):
    high = lax.reduce_precision(values, 8, 7)
    return high.astype(jnp.bfloat16), (values - high).astype(jnp.bfloat16)


def angle_pair(rows, cols, period):
    row_ids = lax.broadcasted_iota(jnp.int32, (rows, cols), 0)
    col_ids = lax.broadcasted_iota(jnp.int32, (rows, cols), 1)
    angles = 2.0 * math.pi / period * (row_ids * col_ids % period).astype(jnp.float32)
    return jnp.cos(angles), jnp.sin(angles)


def lane_table(sign):
    cosine, sine_part = angle_pair(LANES, LANES, LANES)
    sine_part = sign * sine_part
    return split_table(
        jnp.concatenate(
            [
                jnp.concatenate([cosine, sine_part], axis=1),
                jnp.concatenate([-sine_part, cosine], axis=1),
            ],
            axis=0,
        )
    )


def turns(length):
    cosine, sine_part = angle_pair(HALF, LANES, length)
    both = jnp.stack([cosine, sine_part], axis=1).reshape(HALF // 2, 2, 2, LANES)
    return jnp.swapaxes(both, 0, 1)


def column_tables(length):
    cos_b, sin_b = angle_pair(LANES, LANES, LANES)
    cos_c, sin_c = angle_pair(HALF, LANES, length)

    def both(turn_shape, axis):
        ct, st = cos_c.reshape(turn_shape), sin_c.reshape(turn_shape)
        cosine = ct * cos_b - st * sin_b
        sine_part = st * cos_b + ct * sin_b
        return split_table(jnp.concatenate([cosine, -sine_part], axis=axis))

    inverse = both((HALF, 1, LANES), 2)
    forward = both((HALF, LANES, 1), 1)
    return inverse + forward


def fast_term(plan, member, section_field, finish):
    rows, cols, length = plan["rows"], plan["cols"], plan["length"]
    slots, per, home = plan["slots"], plan["per"], plan["home"]
    row = lax.axis_index("row")
    col = lax.axis_index("col")
    where = jnp.stack([row, col * plan["block_x"]]).astype(jnp.int32)
    info = jnp.asarray(line_info(plan), jnp.int32)[col]
    info = info + jnp.where(jnp.arange(slots + 2) < slots, row * SUBL, 0).astype(jnp.int32)
    more = (home - per) * LANES
    edge = jnp.where(
        row < rows // 2, section_field[member, :, :, per * LANES:],
        section_field[member, :, :, :more],
    )
    got = lax.ppermute(edge, "row", [(0, 1), (3, 2)])
    own, moved = pack(plan, where, section_field, member, got)

    def swap(lines):
        return lax.all_to_all(lines, "row", split_axis=0, concat_axis=0, tiled=True)

    def across(lines):
        return lax.all_to_all(lines, ("col", "row"), split_axis=0, concat_axis=0, tiled=True)

    pairs = [[(d, t) for d, t, turn in plan["moves"] if turn == k] for k in range(2)]
    moved1 = lax.ppermute(moved, "col", pairs[0])
    moved2 = lax.ppermute(moved, "col", pairs[1])
    own = swap(own)
    moved1 = swap(moved1)
    moved2 = swap(moved2)
    turn = turns(length)
    table = lane_table(1.0)
    spread = [
        across(lines_in(plan, parity, info, own, moved1, moved2, turn[parity], table))
        for parity in range(2)
    ]
    tables = column_tables(length)
    back = [across(columns(plan, part, tables)) for part in spread]
    own, moved1, moved2 = lines_out(plan, info, *back, turn, lane_table(-1.0))
    own = swap(own)
    moved1 = swap(moved1)
    moved2 = swap(moved2)
    flip = [[(t, d) for d, t in group] for group in pairs]
    moved = lax.ppermute(moved1, "col", flip[0]) + lax.ppermute(moved2, "col", flip[1])

    def edge_of(lines):
        side = jnp.where(row < rows // 2, lines[..., :more], lines[..., per * LANES - more:])
        return lax.ppermute(side, "row", [(1, 0), (2, 3)])

    return finish(where, own, moved, edge_of(own), edge_of(moved))


def fast_device(plan, start_field, section_field, start_term, first_term, second_term):
    wave_x, wave_y = positions(
        (plan["block_x"], plan["block_y"]),
        lax.axis_index("col") * plan["block_x"],
        lax.axis_index("row") * plan["block_y"],
        plan["length"],
    )
    damping, weight_a, weight_b, weight_c = section_weights(wave_x, wave_y, plan["length"])[:4]
    linear = (
        damping * start_field
        + weight_a * start_term
        + 2.0 * weight_b * (first_term + second_term)
    )
    linear, weight_c = lax.optimization_barrier((linear, weight_c))
    out = []
    for member in range(start_field.shape[0]):
        out.append(
            fast_term(
                plan, member, section_field,
                lambda where, *parts: unpack(plan, where, *parts, linear[member], weight_c),
            )
        )
    return jnp.stack(out)


def solution(mesh):
    rows, cols = mesh.shape["row"], mesh.shape["col"]

    def body(start_field, *rest):
        block_x, block_y = start_field.shape[2], start_field.shape[3]
        plan = plan_of(block_y * rows, rows, cols, block_x, block_y)
        if plan is None:
            return per_device(start_field, *rest)
        return fast_device(plan, start_field, *rest)

    return jax.shard_map(
        body,
        mesh=mesh,
        in_specs=(P(None, None, "col", "row"),) * 5,
        out_specs=P(None, None, "col", "row"),
        check_vma=False,
    )
```

```python
import functools
import math

import jax
import jax.numpy as jnp
from jax import lax
from jax.experimental import pallas as pl
from jax.experimental.pallas import tpu as pltpu
from jax.sharding import PartitionSpec as P

RADIX = 128


viscous_rate = 1.5
wave_scale = 3.0
series_terms = 12


def section_weights(wave_x, wave_y, length):
    square = wave_x * wave_x + wave_y * wave_y
    kappa_x = wave_scale * wave_x.astype(jnp.float32) / length
    kappa_y = wave_scale * wave_y.astype(jnp.float32) / length
    kappa_sq = kappa_x * kappa_x + kappa_y * kappa_y
    zvalue = -viscous_rate * kappa_sq
    damping = jnp.exp(zvalue)
    near_zero = 27 * square < 2 * length * length

    def series(degree):
        running = jnp.full_like(zvalue, 1.0 / math.factorial(series_terms - 1 + degree))
        for term_index in range(series_terms - 2, -1, -1):
            running = running * zvalue + 1.0 / math.factorial(term_index + degree)
        return running

    clamped = jnp.where(near_zero, -1.0, zvalue)
    exp_clamped = jnp.exp(clamped)
    closed_one = (exp_clamped - 1.0) / clamped
    closed_two = (exp_clamped - 1.0 - clamped) / (clamped * clamped)
    closed_three = (exp_clamped - 1.0 - clamped - 0.5 * clamped * clamped) / (
        clamped * clamped * clamped
    )
    phi_one = jnp.where(near_zero, series(1), closed_one)
    phi_two = jnp.where(near_zero, series(2), closed_two)
    phi_three = jnp.where(near_zero, series(3), closed_three)
    weight_a = phi_one - 3.0 * phi_two + 4.0 * phi_three
    weight_b = phi_two - 2.0 * phi_three
    weight_c = 4.0 * phi_three - phi_two
    keep_mask = ((3 * jnp.abs(wave_x) < length) & (3 * jnp.abs(wave_y) < length)).astype(
        jnp.float32
    )
    inverse_sq = length * length / (9.0 * jnp.maximum(square, 1).astype(jnp.float32))
    return (damping, weight_a, weight_b, weight_c, kappa_x, kappa_y, keep_mask, inverse_sq)


def section_table(count_in, count_out, period, direction):
    row_ids = lax.broadcasted_iota(jnp.int32, (count_in, count_out), 0)
    col_ids = lax.broadcasted_iota(jnp.int32, (count_in, count_out), 1)
    angles = direction * 2.0 * math.pi / period * (row_ids * col_ids % period).astype(jnp.float32)
    cosine = jnp.cos(angles)
    sine_part = jnp.sin(angles)
    return jnp.stack(
        [jnp.stack([cosine, sine_part], axis=1), jnp.stack([-sine_part, cosine], axis=1)], axis=0
    )


def twiddle(count_c, count_b, period, direction):
    row_ids = lax.broadcasted_iota(jnp.int32, (count_c, count_b), 0)
    col_ids = lax.broadcasted_iota(jnp.int32, (count_c, count_b), 1)
    angles = direction * 2.0 * math.pi / period * (row_ids * col_ids % period).astype(jnp.float32)
    return (jnp.cos(angles), jnp.sin(angles))


def rotate(values, cosine, sine_part):
    return jnp.stack(
        [values[0] * cosine - values[1] * sine_part, values[0] * sine_part + values[1] * cosine]
    )


def product(equation, left, right):
    return jnp.einsum(equation, left, right, precision=lax.Precision.HIGH)


def lines_inverse(pieces):
    parts, count_k, length = pieces.shape
    count_b = RADIX
    count_a = length // count_b
    shaped = pieces.reshape((parts, count_k, count_a, count_b))
    first = product("pkab,pasc->skcb", shaped, section_table(count_a, count_a, count_a, 1.0))
    first = rotate(first, *twiddle(count_a, count_b, length, 1.0))
    second = product("pkcb,pbsd->skcd", first, section_table(count_b, count_b, count_b, 1.0))
    return second.reshape((parts, count_k, length))


def lines_forward(pieces):
    parts, count_k, length = pieces.shape
    count_d = RADIX
    count_c = length // count_d
    shaped = pieces.reshape((parts, count_k, count_c, count_d))
    first = product("pkcd,pdsf->skcf", shaped, section_table(count_d, count_d, count_d, -1.0))
    first = rotate(first, *twiddle(count_c, count_d, length, -1.0))
    second = product("pkcf,pcse->skef", first, section_table(count_c, count_c, count_c, -1.0))
    return second.reshape((parts, count_k, length))


def turned_table(count_c, count_b, period, direction):
    c_ids = lax.broadcasted_iota(jnp.int32, (count_c, count_b, count_b), 0)
    b_ids = lax.broadcasted_iota(jnp.int32, (count_c, count_b, count_b), 1)
    d_ids = lax.broadcasted_iota(jnp.int32, (count_c, count_b, count_b), 2)
    steps = b_ids * (c_ids + count_c * d_ids) % period
    angles = direction * 2.0 * math.pi / period * steps.astype(jnp.float32)
    return jnp.cos(angles), jnp.sin(angles)


def columns_inverse(pieces, table):
    parts, half_count, count_y = pieces.shape
    count_a = half_count // RADIX
    count_c = 2 * count_a
    shaped = pieces.reshape((parts, count_a, RADIX, count_y))
    first = product("paby,pasc->csby", shaped, section_table(count_a, count_c, count_c, 1.0))
    return product("csby,csbd->cdy", first, table)


def columns_forward(grid, table):
    count_c, count_d, count_y = grid.shape
    half_count = count_c // 2
    first = product("cdy,cpfd->cpfy", grid, table)
    second = product(
        "cpfy,pcse->sefy", first, section_table(count_c, half_count, count_c, -1.0)
    )
    return second.reshape((2, half_count * count_d, count_y))


def to_columns(lines):
    return lax.all_to_all(lines, ("col", "row"), split_axis=2, concat_axis=1, tiled=True)


def to_lines(columns):
    return lax.all_to_all(columns, ("col", "row"), split_axis=1, concat_axis=2, tiled=True)


def positions(shape, start_x, start_y, length):
    wave_x = start_x + lax.broadcasted_iota(jnp.int32, shape, 0)
    index_y = start_y + lax.broadcasted_iota(jnp.int32, shape, 1)
    wave_y = jnp.where(index_y < length // 2, index_y, index_y - length)
    return wave_x, wave_y


def nonlinear(section_field, length):
    block_x = section_field.shape[1]
    lines = lax.all_to_all(section_field, "row", split_axis=1, concat_axis=2, tiled=True)
    count_k = lines.shape[1]
    start_x = lax.axis_index("col") * block_x + lax.axis_index("row") * count_k
    wave_x, wave_y = positions((count_k, length), start_x, 0, length)
    square = wave_x * wave_x + wave_y * wave_y
    kappa_x = wave_scale * wave_x.astype(jnp.float32) / length
    kappa_y = wave_scale * wave_y.astype(jnp.float32) / length
    keep = (3 * jnp.abs(wave_x) < length) & (3 * jnp.abs(wave_y) < length)
    doubled = jnp.where(wave_x == 0, 1.0, 2.0) * (1.0 / length)
    inverse_sq = length * length / (9.0 * jnp.maximum(square, 1).astype(jnp.float32))
    factor = jnp.where(keep, inverse_sq * doubled, 0.0)
    scale_u = kappa_y * factor
    scale_v = kappa_x * factor
    spec_u = jnp.stack([-scale_u * lines[1], scale_u * lines[0]])
    spec_v = jnp.stack([scale_v * lines[1], -scale_v * lines[0]])
    count_c = length // RADIX
    cosine, sine_part = turned_table(count_c, RADIX, length, 1.0)
    table = jnp.stack([cosine, -sine_part], axis=1)
    vel_u = columns_inverse(to_columns(lines_inverse(spec_u)), table)
    vel_v = columns_inverse(to_columns(lines_inverse(spec_v)), table)
    cross = lines_forward(to_lines(columns_forward(vel_u * vel_v, table)))
    square_gap = lines_forward(
        to_lines(columns_forward((vel_v - vel_u) * (vel_v + vel_u), table))
    )
    scale = jnp.where(keep, 1.0 / length, 0.0)
    weight_cross = (kappa_x * kappa_x - kappa_y * kappa_y) * scale
    weight_gap = kappa_x * kappa_y * scale
    term = weight_cross * cross + weight_gap * square_gap
    return lax.all_to_all(term, "row", split_axis=2, concat_axis=1, tiled=True)


def per_device(start_field, section_field, start_term, first_term, second_term):
    members = start_field.shape[0]
    block_x = start_field.shape[2]
    block_y = start_field.shape[3]
    length = block_y * lax.axis_size("row")
    wave_x, wave_y = positions(
        (block_x, block_y),
        lax.axis_index("col") * block_x,
        lax.axis_index("row") * block_y,
        length,
    )
    damping, weight_a, weight_b, weight_c = section_weights(wave_x, wave_y, length)[:4]
    linear = (
        damping * start_field
        + weight_a * start_term
        + 2.0 * weight_b * (first_term + second_term)
    )
    linear, weight_c = lax.optimization_barrier((linear, weight_c))
    section_term = jnp.stack([nonlinear(section_field[m], length) for m in range(members)])
    return linear + weight_c * section_term


LANES = 128
SUBL = 8
HALF = 64


def plan_of(length, rows, cols, block_x, block_y):
    if length != LANES * HALF or rows != 4 or block_x % (rows * SUBL) or block_y * rows != length:
        return None
    kept = (length - 1) // 3 + 1
    stride = rows * SUBL
    groups = block_x // stride
    own = [min(groups, max(0, -(-(kept - c * block_x) // stride))) for c in range(cols)]
    slots = -(-sum(own) // cols)
    extra = groups - slots
    donors = [c for c in range(cols) if own[c] == groups]
    if extra <= 0 or 2 * extra > slots or any(slots < own[c] < groups for c in range(cols)):
        return None
    takers = [c for c in range(cols) if own[c] + extra <= slots]
    first = [(c, 0) for c in takers]
    second = [(c, 1) for c in takers if own[c] == 0]
    places = first + second
    if len(donors) > len(places):
        return None
    order = donors[-1:] + donors[:-1]
    moves = [(donor, taker, turn) for donor, (taker, turn) in zip(order, places)]
    low = (kept + LANES - 1) // LANES
    high = HALF - (length - kept + 1) // LANES
    if low != high or low % 2 or low > HALF // 2:
        return None
    if not block_y < low * LANES < 2 * block_y or block_y % LANES:
        return None
    return dict(
        kept=kept, stride=stride, groups=groups, own=own, slots=slots, extra=extra,
        moves=moves, low=low, rows=rows, cols=cols,
        block_x=block_x, block_y=block_y, length=length,
    )


def home_of(plan, group):
    per_block = plan["block_x"] // SUBL
    if group * SUBL >= plan["kept"]:
        return None
    col, inside = divmod(group, per_block)
    slot = inside // plan["rows"]
    if slot < plan["slots"]:
        return col, slot
    for donor, taker, turn in plan["moves"]:
        if donor == col:
            start = plan["slots"] - plan["extra"] if turn == 0 else 0
            return taker, start + slot - plan["slots"]
    raise ValueError("no place")


def line_info(plan):
    rows = []
    slots, extra = plan["slots"], plan["extra"]
    for col in range(plan["cols"]):
        base = [col * plan["block_x"] + slot * plan["stride"] for slot in range(slots)]
        for donor, taker, turn in plan["moves"]:
            if taker == col:
                start = slots - extra if turn == 0 else 0
                for step in range(extra):
                    base[start + step] = donor * plan["block_x"] + (slots + step) * plan["stride"]
        rows.append(base)
    return rows


def cadd(a, b):
    if a is None:
        return b
    if b is None:
        return a
    return (a[0] + b[0], a[1] + b[1])


def csub(a, b):
    if b is None:
        return a
    if a is None:
        return (-b[0], -b[1])
    return (a[0] - b[0], a[1] - b[1])


def cturn(a, step, period, sign):
    if a is None:
        return None
    step = step * sign % period
    if step == 0:
        return a
    if 4 * step == period:
        return (-a[1], a[0])
    if 2 * step == period:
        return (-a[0], -a[1])
    if 4 * step == 3 * period:
        return (a[1], -a[0])
    angle = 2.0 * math.pi * step / period
    cosine, sine_part = math.cos(angle), math.sin(angle)
    if 8 * step % period == 0:
        size = math.sqrt(0.5)
        sign_c, sign_s = (1 if cosine > 0 else -1), (1 if sine_part > 0 else -1)
        real = a[0] - a[1] if sign_c == sign_s else a[0] + a[1]
        imag = a[0] + a[1] if sign_c == sign_s else a[1] - a[0]
        return (real * (sign_c * size), imag * (sign_c * size))
    return (a[0] * cosine - a[1] * sine_part, a[0] * sine_part + a[1] * cosine)


def butterflies(values, sign, need):
    count = len(values)
    if all(v is None for v in values):
        return {k: None for k in need}
    if count == 1:
        return {k: values[0] for k in need}
    half = count // 2
    sub = sorted({k % half for k in need})
    even = butterflies(values[0::2], sign, sub)
    odd = butterflies(values[1::2], sign, sub)
    wanted = set(need)
    out = {}
    for k in sub:
        turned = cturn(odd[k], k, count, sign)
        if k in wanted:
            out[k] = cadd(even[k], turned)
        if k + half in wanted:
            out[k + half] = csub(even[k], turned)
    return out


def halves(values):
    high = values.astype(jnp.bfloat16)
    return high, (values - high.astype(jnp.float32)).astype(jnp.bfloat16)


def dot3(left, right):
    lh, ll = left
    rh, rl = right
    def mm(a, b):
        return jnp.dot(a, b, preferred_element_type=jnp.float32)
    return mm(lh, rh) + (mm(ll, rh) + mm(lh, rl))


def tile_of(plan, a):
    low = plan["low"]
    return LANES * (a if a < low else a - (HALF - 2 * low))


def kept_tiles(plan):
    low = plan["low"]
    return list(range(low)) + list(range(HALF - low, HALF))


def sublane_iota():
    return lax.broadcasted_iota(jnp.int32, (SUBL, LANES), 0)


def lane_iota():
    return lax.broadcasted_iota(jnp.int32, (SUBL, LANES), 1)


def keep_of(plan, wave_x, wave_y):
    return (3 * wave_x < plan["length"]) & (3 * jnp.abs(wave_y) < plan["length"])


def lines_in_kernel(plan, parity, info, lines, turn, wh, wl, out, scr):
    length = plan["length"]
    j = pl.program_id(0)
    wave_x = info[j] + sublane_iota()
    kx = wave_x.astype(jnp.float32)
    doubled = jnp.where(wave_x == 0, 1.0, 2.0) * (length / 9.0)
    step = wave_scale / length
    lane = lane_iota()
    for field in range(2):
        tiles = {}
        for a in kept_tiles(plan):
            off = tile_of(plan, a)
            wave_y = lane + (LANES * a - (length if a >= HALF // 2 else 0))
            square = (wave_x * wave_x + wave_y * wave_y)
            factor = doubled / jnp.maximum(square, 1).astype(jnp.float32)
            keep = keep_of(plan, wave_x, wave_y)
            if field == 0:
                factor = factor * (step * wave_y.astype(jnp.float32))
            else:
                factor = factor * (-step * kx)
            parts = []
            for p in range(2):
                parts.append(jnp.where(keep, lines[p, 0, :, off:off + LANES], 0.0))
            tiles[a] = (-factor * parts[1], factor * parts[0])
        mixed = []
        for a in range(HALF // 2):
            x0, x1 = tiles.get(a), tiles.get(a + HALF // 2)
            if parity == 0:
                mixed.append(cadd(x0, x1))
            else:
                mixed.append(cturn(csub(x0, x1), a, HALF, 1))
        result = butterflies(mixed, 1, range(HALF // 2))
        for e in range(HALF // 2):
            re, im = result[e]
            cosine, sine_part = turn[e, 0:1, :], turn[e, 1:2, :]
            at = slice(SUBL * e, SUBL * (e + 1))
            scr[at, 0:LANES] = re * cosine - im * sine_part
            scr[at, LANES:] = re * sine_part + im * cosine
        spread = dot3(halves(scr[...]), (wh[...], wl[...]))
        for s in range(2):
            out[:, field, s] = spread[:, s * LANES:(s + 1) * LANES].reshape(
                HALF // 2, SUBL, LANES
            )


def lines_in(plan, parity, info, lines, turn, table):
    slots = plan["slots"]
    width = 2 * plan["low"] * LANES
    devices = plan["rows"] * plan["cols"]
    whole = lambda shape: pl.BlockSpec(shape, lambda j: (0,) * len(shape))
    return pl.pallas_call(
        functools.partial(lines_in_kernel, plan, parity),
        grid=(slots,),
        in_specs=[
            pl.BlockSpec(memory_space=pltpu.SMEM),
            pl.BlockSpec((2, 1, SUBL, width), lambda j: (0, j, 0, 0)),
            whole((HALF // 2, 2, LANES)),
            whole((2 * LANES, 2 * LANES)),
            whole((2 * LANES, 2 * LANES)),
        ],
        out_specs=pl.BlockSpec((devices, 2, 2, SUBL, LANES), lambda j: (0, 0, 0, j, 0)),
        out_shape=jax.ShapeDtypeStruct((devices, 2, 2, slots * SUBL, LANES), jnp.float32),
        scratch_shapes=[pltpu.VMEM((HALF // 2 * SUBL, 2 * LANES), jnp.float32)],
        compiler_params=pltpu.CompilerParams(vmem_limit_bytes=60 << 20),
        cost_estimate=pl.CostEstimate(flops=4 << 30, bytes_accessed=16 << 20, transcendentals=0),
        name="lines_in",
    )(info, lines, turn, *table)


def columns_kernel(plan, src, th, tl, fh, fl, out, mid):
    rows = plan["rows"]
    low = plan["low"]
    per_tile = LANES // SUBL
    quarter = per_tile // rows
    inside = [[home_of(plan, a * per_tile + q * rows) for a in range(low)] for q in range(quarter)]
    used = {place for line in inside for place in line if place}

    @pl.loop(0, 2 * rows)
    def _(i):
        r = i % rows
        field = i // rows
        lanes = pl.ds(pl.multiple_of(field * LANES, LANES), LANES)
        for q in range(quarter):
            values = []
            for a in range(HALF):
                place = inside[q][a] if a < low else None
                if place is None:
                    values.append(None)
                    continue
                at = pl.ds(place[1] * SUBL, SUBL)
                dev = place[0] * rows + r
                values.append((src[dev, field, 0, at, :], src[dev, field, 1, at, :]))
            result = butterflies(values, 1, range(HALF))
            base = pl.multiple_of((q * rows + r) * SUBL, SUBL)
            for c in range(HALF):
                mid[c, pl.ds(base, SUBL), lanes] = result[c][0]
                mid[c, pl.ds(LANES + base, SUBL), lanes] = result[c][1]

    @pl.loop(0, HALF)
    def _(c):
        grid = dot3((th[c], tl[c]), halves(mid[c]))
        u, v = grid[:, :LANES], grid[:, LANES:]
        pair = jnp.concatenate([u * v, (v - u) * (v + u)], axis=1)
        mid[c] = dot3((fh[c], fl[c]), halves(pair))

    @pl.loop(0, 2 * rows)
    def _(i):
        r = i % rows
        field = i // rows
        lanes = pl.ds(pl.multiple_of(field * LANES, LANES), LANES)
        for q in range(quarter):
            base = pl.multiple_of((q * rows + r) * SUBL, SUBL)
            values = [
                (mid[c, pl.ds(base, SUBL), lanes], mid[c, pl.ds(LANES + base, SUBL), lanes])
                for c in range(HALF)
            ]
            need = [a for a in range(low) if inside[q][a]]
            result = butterflies(values, -1, need)
            for a in need:
                place = inside[q][a]
                at = pl.ds(place[1] * SUBL, SUBL)
                dev = place[0] * rows + r
                out[dev, field, 0, at, :] = result[a][0]
                out[dev, field, 1, at, :] = result[a][1]
        for col in range(plan["cols"]):
            for slot in range(plan["slots"]):
                if (col, slot) not in used:
                    for p in range(2):
                        out[col * rows + r, field, p, pl.ds(slot * SUBL, SUBL), :] = jnp.zeros(
                            (SUBL, LANES), jnp.float32
                        )


def columns(plan, spread, tables):
    return pl.pallas_call(
        functools.partial(columns_kernel, plan),
        in_specs=[pl.BlockSpec(memory_space=pltpu.VMEM)] * 5,
        out_specs=pl.BlockSpec(memory_space=pltpu.VMEM),
        out_shape=jax.ShapeDtypeStruct(spread.shape, jnp.float32),
        scratch_shapes=[pltpu.VMEM((HALF, 2 * LANES, 2 * LANES), jnp.float32)],
        compiler_params=pltpu.CompilerParams(vmem_limit_bytes=60 << 20),
        cost_estimate=pl.CostEstimate(flops=16 << 30, bytes_accessed=30 << 20, transcendentals=0),
        name="columns",
    )(spread, *tables)


def lines_out_kernel(plan, info, got0, got1, turn, wh, wl, lines, scr, acc):
    length = plan["length"]
    j = pl.program_id(0)
    wave_x = info[j] + sublane_iota()
    step = wave_scale / length
    kappa_x = step * wave_x.astype(jnp.float32)
    lane = lane_iota()
    tiles = kept_tiles(plan)
    rows = HALF // 2 * SUBL
    for field in range(2):
        for parity, got in enumerate((got0, got1)):
            both = jnp.concatenate(
                [got[:, field, s].reshape(rows, LANES) for s in range(2)], axis=1
            )
            scr[parity] = dot3(halves(both), (wh[...], wl[...]))
        values = []
        for c in range(HALF):
            e, parity = c // 2, c % 2
            at = slice(SUBL * e, SUBL * (e + 1))
            re, im = scr[parity, at, 0:LANES], scr[parity, at, LANES:]
            cosine, sine_part = turn[parity, e, 0:1, :], turn[parity, e, 1:2, :]
            values.append((re * cosine + im * sine_part, im * cosine - re * sine_part))
        result = butterflies(values, -1, tiles)
        for t, a in enumerate(tiles):
            wave_y = lane + (LANES * a - (length if a >= HALF // 2 else 0))
            kappa_y = step * wave_y.astype(jnp.float32)
            keep = keep_of(plan, wave_x, wave_y)
            if field == 0:
                weight = (kappa_x * kappa_x - kappa_y * kappa_y) * (1.0 / length)
            else:
                weight = kappa_x * kappa_y * (1.0 / length)
            off = tile_of(plan, a)
            for p in range(2):
                value = jnp.where(keep, weight * result[a][p], 0.0)
                if field == 0:
                    acc[t, p] = value
                else:
                    lines[p, 0, :, off:off + LANES] = acc[t, p] + value


def lines_out(plan, info, got0, got1, turn, table):
    slots = plan["slots"]
    width = 2 * plan["low"] * LANES
    devices = plan["rows"] * plan["cols"]
    whole = lambda shape: pl.BlockSpec(shape, lambda j: (0,) * len(shape))
    got_spec = pl.BlockSpec((devices, 2, 2, SUBL, LANES), lambda j: (0, 0, 0, j, 0))
    return pl.pallas_call(
        functools.partial(lines_out_kernel, plan),
        grid=(slots,),
        in_specs=[
            pl.BlockSpec(memory_space=pltpu.SMEM),
            got_spec,
            got_spec,
            whole((2, HALF // 2, 2, LANES)),
            whole((2 * LANES, 2 * LANES)),
            whole((2 * LANES, 2 * LANES)),
        ],
        out_specs=pl.BlockSpec((2, 1, SUBL, width), lambda j: (0, j, 0, 0)),
        out_shape=jax.ShapeDtypeStruct((2, slots, SUBL, width), jnp.float32),
        scratch_shapes=[
            pltpu.VMEM((2, HALF // 2 * SUBL, 2 * LANES), jnp.float32),
            pltpu.VMEM((2 * plan["low"], 2, SUBL, LANES), jnp.float32),
        ],
        compiler_params=pltpu.CompilerParams(vmem_limit_bytes=60 << 20),
        cost_estimate=pl.CostEstimate(flops=8 << 30, bytes_accessed=22 << 20, transcendentals=0),
        name="lines_out",
    )(info, got0, got1, turn, *table)


def spans(plan, row):
    full = plan["block_y"]
    short = plan["low"] * LANES - full
    side, inner = row // 2, row % 2

    def at(offset):
        return pl.multiple_of(offset, LANES)

    return (
        (at(side * (full - short)), at(side * (full + short) + inner * full), short),
        (at((1 - side) * short), at(short + side * (full + short)), full - short),
    )


def both_of(row):
    return row // 2 == row % 2


def own_cases(plan):
    cases = []
    for col, count in enumerate(plan["own"]):
        count = min(count, plan["slots"])
        if not count:
            continue
        if cases and cases[-1][2] == count:
            cases[-1] = (cases[-1][0], col, count)
        else:
            cases.append((col, col, count))
    return cases


def exchange_kernel(plan, back, source, target, send, recv):
    rows, slots, extra = plan["rows"], plan["slots"], plan["extra"]
    row, col = lax.axis_index("row"), lax.axis_index("col")

    def views(home, lines, begin, count, start, line_row, home_row, piece):
        home_at, line_at, width = spans(plan, home_row)[piece]
        return (
            home.at[:, pl.ds(begin, count), line_row, :, pl.ds(home_at, width)],
            lines.at[:, pl.ds(start, count), :, pl.ds(line_at, width)],
        )

    def copy(kind, step, piece, begin, count, start, where, line_row, home_row, turn):
        if back:
            dst, src = views(target, source, begin, count, start, line_row, home_row, piece)
        else:
            src, dst = views(source, target, begin, count, start, line_row, home_row, piece)
        if where is None:
            return pltpu.make_async_copy(src, dst, send.at[kind, step, piece])
        return pltpu.make_async_remote_copy(
            src_ref=src, dst_ref=dst, send_sem=send.at[kind + turn, step, piece],
            recv_sem=recv.at[kind + turn, step, piece], device_id=where,
            device_id_type=pl.DeviceIdType.MESH,
        )

    def each(home_row, act):
        act(0)

        @pl.when(both_of(home_row))
        def _():
            act(1)

    def moved(verb):
        for donor, taker, turn in plan["moves"]:
            start = slots - extra if turn == 0 else 0
            sender, receiver = (taker, donor) if back else (donor, taker)
            peer = sender if verb == "recv" else receiver

            @pl.when(col == (receiver if verb == "recv" else sender))
            def _():
                for step in range(rows):
                    other = (row + step) % rows if verb != "recv" else (row + rows - step) % rows
                    mine_is_line = back == (verb != "recv")
                    line_row, home_row = (row, other) if mine_is_line else (other, row)

                    def act(piece):
                        it = copy(
                            1, step, piece, slots, extra, start,
                            {"col": peer, "row": other}, line_row, home_row, turn,
                        )
                        do(it, verb)

                    each(home_row, act)

    def do(it, verb):
        if verb == "start":
            it.start()
        elif verb == "send":
            it.wait_send()
        else:
            it.wait_recv()

    def owned(verb):
        for first, last, count in own_cases(plan):
            @pl.when((col >= first) & (col <= last))
            def _():
                for step in range(1, rows):
                    other = (row + step) % rows if verb != "recv" else (row + rows - step) % rows
                    mine_is_line = back == (verb != "recv")
                    line_row, home_row = (row, other) if mine_is_line else (other, row)

                    def act(piece):
                        do(
                            copy(
                                0, step, piece, 0, count, 0, {"row": other}, line_row,
                                home_row, 0,
                            ),
                            verb,
                        )

                    each(home_row, act)

    def local(verb):
        for first, last, count in own_cases(plan):
            @pl.when((col >= first) & (col <= last))
            def _():
                def act(piece):
                    it = copy(0, 0, piece, 0, count, 0, None, row, row, 0)
                    if verb == "start":
                        it.start()
                    else:
                        it.wait()

                each(row, act)

    moved("start")
    owned("start")
    local("start")
    local("wait")
    owned("recv")
    moved("recv")
    owned("send")
    moved("send")


def exchange(plan, back, source):
    rows, groups = plan["rows"], plan["groups"]
    home = (2, groups, rows, SUBL, plan["block_y"])
    lines = (2, plan["slots"], SUBL, 2 * plan["low"] * LANES)
    turns_used = 3
    return pl.pallas_call(
        functools.partial(exchange_kernel, plan, back),
        in_specs=[pl.BlockSpec(memory_space=pl.ANY)],
        out_specs=pl.BlockSpec(memory_space=pl.ANY),
        out_shape=jax.ShapeDtypeStruct(home if back else lines, jnp.float32),
        scratch_shapes=[
            pltpu.SemaphoreType.DMA((turns_used, rows, 2)),
            pltpu.SemaphoreType.DMA((turns_used, rows, 2)),
        ],
        compiler_params=pltpu.CompilerParams(has_side_effects=True, vmem_limit_bytes=60 << 20),
        cost_estimate=pl.CostEstimate(flops=1 << 34, bytes_accessed=16 << 20, transcendentals=0),
        name="lines_home" if back else "home_lines",
    )(source)


def split_table(values):
    high = lax.reduce_precision(values, 8, 7)
    return high.astype(jnp.bfloat16), (values - high).astype(jnp.bfloat16)


def angle_pair(rows, cols, period):
    row_ids = lax.broadcasted_iota(jnp.int32, (rows, cols), 0)
    col_ids = lax.broadcasted_iota(jnp.int32, (rows, cols), 1)
    angles = 2.0 * math.pi / period * (row_ids * col_ids % period).astype(jnp.float32)
    return jnp.cos(angles), jnp.sin(angles)


def lane_table(sign):
    cosine, sine_part = angle_pair(LANES, LANES, LANES)
    sine_part = sign * sine_part
    return split_table(
        jnp.concatenate(
            [
                jnp.concatenate([cosine, sine_part], axis=1),
                jnp.concatenate([-sine_part, cosine], axis=1),
            ],
            axis=0,
        )
    )


def turns(length):
    cosine, sine_part = angle_pair(HALF, LANES, length)
    both = jnp.stack([cosine, sine_part], axis=1).reshape(HALF // 2, 2, 2, LANES)
    return jnp.swapaxes(both, 0, 1)


def column_tables(length):
    cos_b, sin_b = angle_pair(LANES, LANES, LANES)
    cos_c, sin_c = angle_pair(HALF, LANES, length)

    def both(turn_shape, axis):
        ct, st = cos_c.reshape(turn_shape), sin_c.reshape(turn_shape)
        cosine = ct * cos_b - st * sin_b
        sine_part = st * cos_b + ct * sin_b
        return split_table(jnp.concatenate([cosine, -sine_part], axis=axis))

    inverse = both((HALF, 1, LANES), 2)
    forward = both((HALF, LANES, 1), 1)
    return inverse + forward


def fast_term(plan, field):
    rows = plan["rows"]
    row, col = lax.axis_index("row"), lax.axis_index("col")
    info = jnp.asarray(line_info(plan), jnp.int32)[col] + (row * SUBL).astype(jnp.int32)

    def across(lines):
        return lax.all_to_all(lines, ("col", "row"), split_axis=0, concat_axis=0, tiled=True)

    home = field.reshape(2, plan["groups"], rows, SUBL, plan["block_y"])
    lines = exchange(plan, False, home)
    turn = turns(plan["length"])
    table = lane_table(1.0)
    spread = [
        across(lines_in(plan, parity, info, lines, turn[parity], table)) for parity in range(2)
    ]
    tables = column_tables(plan["length"])
    back = [across(columns(plan, part, tables)) for part in spread]
    lines = lines_out(plan, info, *back, turn, lane_table(-1.0))
    return exchange(plan, True, lines).reshape(field.shape)


def fast_device(plan, start_field, section_field, start_term, first_term, second_term):
    wave_x, wave_y = positions(
        (plan["block_x"], plan["block_y"]),
        lax.axis_index("col") * plan["block_x"],
        lax.axis_index("row") * plan["block_y"],
        plan["length"],
    )
    damping, weight_a, weight_b, weight_c = section_weights(wave_x, wave_y, plan["length"])[:4]
    linear = (
        damping * start_field
        + weight_a * start_term
        + 2.0 * weight_b * (first_term + second_term)
    )
    linear, weight_c = lax.optimization_barrier((linear, weight_c))
    term = jnp.stack([fast_term(plan, section_field[m]) for m in range(start_field.shape[0])])
    keep = keep_of(plan, wave_x, wave_y)
    return linear + jnp.where(keep, weight_c * term, 0.0)


def solution(mesh):
    rows, cols = mesh.shape["row"], mesh.shape["col"]

    def body(start_field, *rest):
        block_x, block_y = start_field.shape[2], start_field.shape[3]
        plan = plan_of(block_y * rows, rows, cols, block_x, block_y)
        if plan is None:
            return per_device(start_field, *rest)
        return fast_device(plan, start_field, *rest)

    return jax.shard_map(
        body,
        mesh=mesh,
        in_specs=(P(None, None, "col", "row"),) * 5,
        out_specs=P(None, None, "col", "row"),
        check_vma=False,
    )
```

```python
import functools
import math

import jax
import jax.numpy as jnp
from jax import lax
from jax.experimental import pallas as pl
from jax.experimental.pallas import tpu as pltpu
from jax.sharding import PartitionSpec as P

RADIX = 128


viscous_rate = 1.5
wave_scale = 3.0
series_terms = 12


def section_weights(wave_x, wave_y, length):
    square = wave_x * wave_x + wave_y * wave_y
    kappa_x = wave_scale * wave_x.astype(jnp.float32) / length
    kappa_y = wave_scale * wave_y.astype(jnp.float32) / length
    kappa_sq = kappa_x * kappa_x + kappa_y * kappa_y
    zvalue = -viscous_rate * kappa_sq
    damping = jnp.exp(zvalue)
    near_zero = 27 * square < 2 * length * length

    def series(degree):
        running = jnp.full_like(zvalue, 1.0 / math.factorial(series_terms - 1 + degree))
        for term_index in range(series_terms - 2, -1, -1):
            running = running * zvalue + 1.0 / math.factorial(term_index + degree)
        return running

    clamped = jnp.where(near_zero, -1.0, zvalue)
    exp_clamped = jnp.exp(clamped)
    closed_one = (exp_clamped - 1.0) / clamped
    closed_two = (exp_clamped - 1.0 - clamped) / (clamped * clamped)
    closed_three = (exp_clamped - 1.0 - clamped - 0.5 * clamped * clamped) / (
        clamped * clamped * clamped
    )
    phi_one = jnp.where(near_zero, series(1), closed_one)
    phi_two = jnp.where(near_zero, series(2), closed_two)
    phi_three = jnp.where(near_zero, series(3), closed_three)
    weight_a = phi_one - 3.0 * phi_two + 4.0 * phi_three
    weight_b = phi_two - 2.0 * phi_three
    weight_c = 4.0 * phi_three - phi_two
    keep_mask = ((3 * jnp.abs(wave_x) < length) & (3 * jnp.abs(wave_y) < length)).astype(
        jnp.float32
    )
    inverse_sq = length * length / (9.0 * jnp.maximum(square, 1).astype(jnp.float32))
    return (damping, weight_a, weight_b, weight_c, kappa_x, kappa_y, keep_mask, inverse_sq)


def section_table(count_in, count_out, period, direction):
    row_ids = lax.broadcasted_iota(jnp.int32, (count_in, count_out), 0)
    col_ids = lax.broadcasted_iota(jnp.int32, (count_in, count_out), 1)
    angles = direction * 2.0 * math.pi / period * (row_ids * col_ids % period).astype(jnp.float32)
    cosine = jnp.cos(angles)
    sine_part = jnp.sin(angles)
    return jnp.stack(
        [jnp.stack([cosine, sine_part], axis=1), jnp.stack([-sine_part, cosine], axis=1)], axis=0
    )


def twiddle(count_c, count_b, period, direction):
    row_ids = lax.broadcasted_iota(jnp.int32, (count_c, count_b), 0)
    col_ids = lax.broadcasted_iota(jnp.int32, (count_c, count_b), 1)
    angles = direction * 2.0 * math.pi / period * (row_ids * col_ids % period).astype(jnp.float32)
    return (jnp.cos(angles), jnp.sin(angles))


def rotate(values, cosine, sine_part):
    return jnp.stack(
        [values[0] * cosine - values[1] * sine_part, values[0] * sine_part + values[1] * cosine]
    )


def product(equation, left, right):
    return jnp.einsum(equation, left, right, precision=lax.Precision.HIGH)


def lines_inverse(pieces):
    parts, count_k, length = pieces.shape
    count_b = RADIX
    count_a = length // count_b
    shaped = pieces.reshape((parts, count_k, count_a, count_b))
    first = product("pkab,pasc->skcb", shaped, section_table(count_a, count_a, count_a, 1.0))
    first = rotate(first, *twiddle(count_a, count_b, length, 1.0))
    second = product("pkcb,pbsd->skcd", first, section_table(count_b, count_b, count_b, 1.0))
    return second.reshape((parts, count_k, length))


def lines_forward(pieces):
    parts, count_k, length = pieces.shape
    count_d = RADIX
    count_c = length // count_d
    shaped = pieces.reshape((parts, count_k, count_c, count_d))
    first = product("pkcd,pdsf->skcf", shaped, section_table(count_d, count_d, count_d, -1.0))
    first = rotate(first, *twiddle(count_c, count_d, length, -1.0))
    second = product("pkcf,pcse->skef", first, section_table(count_c, count_c, count_c, -1.0))
    return second.reshape((parts, count_k, length))


def turned_table(count_c, count_b, period, direction):
    c_ids = lax.broadcasted_iota(jnp.int32, (count_c, count_b, count_b), 0)
    b_ids = lax.broadcasted_iota(jnp.int32, (count_c, count_b, count_b), 1)
    d_ids = lax.broadcasted_iota(jnp.int32, (count_c, count_b, count_b), 2)
    steps = b_ids * (c_ids + count_c * d_ids) % period
    angles = direction * 2.0 * math.pi / period * steps.astype(jnp.float32)
    return jnp.cos(angles), jnp.sin(angles)


def columns_inverse(pieces, table):
    parts, half_count, count_y = pieces.shape
    count_a = half_count // RADIX
    count_c = 2 * count_a
    shaped = pieces.reshape((parts, count_a, RADIX, count_y))
    first = product("paby,pasc->csby", shaped, section_table(count_a, count_c, count_c, 1.0))
    return product("csby,csbd->cdy", first, table)


def columns_forward(grid, table):
    count_c, count_d, count_y = grid.shape
    half_count = count_c // 2
    first = product("cdy,cpfd->cpfy", grid, table)
    second = product(
        "cpfy,pcse->sefy", first, section_table(count_c, half_count, count_c, -1.0)
    )
    return second.reshape((2, half_count * count_d, count_y))


def to_columns(lines):
    return lax.all_to_all(lines, ("col", "row"), split_axis=2, concat_axis=1, tiled=True)


def to_lines(columns):
    return lax.all_to_all(columns, ("col", "row"), split_axis=1, concat_axis=2, tiled=True)


def positions(shape, start_x, start_y, length):
    wave_x = start_x + lax.broadcasted_iota(jnp.int32, shape, 0)
    index_y = start_y + lax.broadcasted_iota(jnp.int32, shape, 1)
    wave_y = jnp.where(index_y < length // 2, index_y, index_y - length)
    return wave_x, wave_y


def nonlinear(section_field, length):
    block_x = section_field.shape[1]
    lines = lax.all_to_all(section_field, "row", split_axis=1, concat_axis=2, tiled=True)
    count_k = lines.shape[1]
    start_x = lax.axis_index("col") * block_x + lax.axis_index("row") * count_k
    wave_x, wave_y = positions((count_k, length), start_x, 0, length)
    square = wave_x * wave_x + wave_y * wave_y
    kappa_x = wave_scale * wave_x.astype(jnp.float32) / length
    kappa_y = wave_scale * wave_y.astype(jnp.float32) / length
    keep = (3 * jnp.abs(wave_x) < length) & (3 * jnp.abs(wave_y) < length)
    doubled = jnp.where(wave_x == 0, 1.0, 2.0) * (1.0 / length)
    inverse_sq = length * length / (9.0 * jnp.maximum(square, 1).astype(jnp.float32))
    factor = jnp.where(keep, inverse_sq * doubled, 0.0)
    scale_u = kappa_y * factor
    scale_v = kappa_x * factor
    spec_u = jnp.stack([-scale_u * lines[1], scale_u * lines[0]])
    spec_v = jnp.stack([scale_v * lines[1], -scale_v * lines[0]])
    count_c = length // RADIX
    cosine, sine_part = turned_table(count_c, RADIX, length, 1.0)
    table = jnp.stack([cosine, -sine_part], axis=1)
    vel_u = columns_inverse(to_columns(lines_inverse(spec_u)), table)
    vel_v = columns_inverse(to_columns(lines_inverse(spec_v)), table)
    cross = lines_forward(to_lines(columns_forward(vel_u * vel_v, table)))
    square_gap = lines_forward(
        to_lines(columns_forward((vel_v - vel_u) * (vel_v + vel_u), table))
    )
    scale = jnp.where(keep, 1.0 / length, 0.0)
    weight_cross = (kappa_x * kappa_x - kappa_y * kappa_y) * scale
    weight_gap = kappa_x * kappa_y * scale
    term = weight_cross * cross + weight_gap * square_gap
    return lax.all_to_all(term, "row", split_axis=2, concat_axis=1, tiled=True)


def per_device(start_field, section_field, start_term, first_term, second_term):
    members = start_field.shape[0]
    block_x = start_field.shape[2]
    block_y = start_field.shape[3]
    length = block_y * lax.axis_size("row")
    wave_x, wave_y = positions(
        (block_x, block_y),
        lax.axis_index("col") * block_x,
        lax.axis_index("row") * block_y,
        length,
    )
    damping, weight_a, weight_b, weight_c = section_weights(wave_x, wave_y, length)[:4]
    linear = (
        damping * start_field
        + weight_a * start_term
        + 2.0 * weight_b * (first_term + second_term)
    )
    linear, weight_c = lax.optimization_barrier((linear, weight_c))
    section_term = jnp.stack([nonlinear(section_field[m], length) for m in range(members)])
    return linear + weight_c * section_term


LANES = 128
SUBL = 8
HALF = 64


def plan_of(length, rows, cols, block_x, block_y):
    if length != LANES * HALF or rows != 4 or block_x % (rows * SUBL) or block_y * rows != length:
        return None
    kept = (length - 1) // 3 + 1
    stride = rows * SUBL
    groups = block_x // stride
    own = [min(groups, max(0, -(-(kept - c * block_x) // stride))) for c in range(cols)]
    slots = -(-sum(own) // cols)
    extra = groups - slots
    donors = [c for c in range(cols) if own[c] == groups]
    if extra <= 0 or 2 * extra > slots or any(slots < own[c] < groups for c in range(cols)):
        return None
    takers = [c for c in range(cols) if own[c] + extra <= slots]
    first = [(c, 0) for c in takers]
    second = [(c, 1) for c in takers if own[c] == 0]
    places = first + second
    if len(donors) > len(places):
        return None
    order = donors[-1:] + donors[:-1]
    moves = [(donor, taker, turn) for donor, (taker, turn) in zip(order, places)]
    low = (kept + LANES - 1) // LANES
    high = HALF - (length - kept + 1) // LANES
    if low != high or low % 2 or low > HALF // 2:
        return None
    if not block_y < low * LANES < 2 * block_y or block_y % LANES:
        return None
    return dict(
        kept=kept, stride=stride, groups=groups, own=own, slots=slots, extra=extra,
        moves=moves, low=low, rows=rows, cols=cols,
        block_x=block_x, block_y=block_y, length=length,
    )


def home_of(plan, group):
    per_block = plan["block_x"] // SUBL
    if group * SUBL >= plan["kept"]:
        return None
    col, inside = divmod(group, per_block)
    slot = inside // plan["rows"]
    if slot < plan["slots"]:
        return col, slot
    for donor, taker, turn in plan["moves"]:
        if donor == col:
            start = plan["slots"] - plan["extra"] if turn == 0 else 0
            return taker, start + slot - plan["slots"]
    raise ValueError("no place")


def first_line(plan, slot):
    slots, extra = plan["slots"], plan["extra"]
    col = lax.axis_index("col")
    base = col * plan["block_x"] + slot * plan["stride"]
    for donor, taker, turn in plan["moves"]:
        start = slots - extra if turn == 0 else 0
        moved = donor * plan["block_x"] + (slots + slot - start) * plan["stride"]
        here = (col == taker) & (slot >= start) & (slot < start + extra)
        base = jnp.where(here, moved, base)
    return base + lax.axis_index("row") * SUBL


def cadd(a, b):
    if a is None:
        return b
    if b is None:
        return a
    return (a[0] + b[0], a[1] + b[1])


def csub(a, b):
    if b is None:
        return a
    if a is None:
        return (-b[0], -b[1])
    return (a[0] - b[0], a[1] - b[1])


def cturn(a, step, period, sign):
    if a is None:
        return None
    step = step * sign % period
    if step == 0:
        return a
    if 4 * step == period:
        return (-a[1], a[0])
    if 2 * step == period:
        return (-a[0], -a[1])
    if 4 * step == 3 * period:
        return (a[1], -a[0])
    angle = 2.0 * math.pi * step / period
    cosine, sine_part = math.cos(angle), math.sin(angle)
    if 8 * step % period == 0:
        size = math.sqrt(0.5)
        sign_c, sign_s = (1 if cosine > 0 else -1), (1 if sine_part > 0 else -1)
        real = a[0] - a[1] if sign_c == sign_s else a[0] + a[1]
        imag = a[0] + a[1] if sign_c == sign_s else a[1] - a[0]
        return (real * (sign_c * size), imag * (sign_c * size))
    return (a[0] * cosine - a[1] * sine_part, a[0] * sine_part + a[1] * cosine)


def butterflies(values, sign, need):
    count = len(values)
    if all(v is None for v in values):
        return {k: None for k in need}
    if count == 1:
        return {k: values[0] for k in need}
    half = count // 2
    sub = sorted({k % half for k in need})
    even = butterflies(values[0::2], sign, sub)
    odd = butterflies(values[1::2], sign, sub)
    wanted = set(need)
    out = {}
    for k in sub:
        turned = cturn(odd[k], k, count, sign)
        if k in wanted:
            out[k] = cadd(even[k], turned)
        if k + half in wanted:
            out[k + half] = csub(even[k], turned)
    return out


def halves(values):
    high = values.astype(jnp.bfloat16)
    return high, (values - high.astype(jnp.float32)).astype(jnp.bfloat16)


def dot3(left, right):
    lh, ll = left
    rh, rl = right
    def mm(a, b):
        return jnp.dot(a, b, preferred_element_type=jnp.float32)
    return mm(lh, rh) + (mm(ll, rh) + mm(lh, rl))


def tile_of(plan, a):
    low = plan["low"]
    return LANES * (a if a < low else a - (HALF - 2 * low))


def kept_tiles(plan):
    low = plan["low"]
    return list(range(low)) + list(range(HALF - low, HALF))


def sublane_iota():
    return lax.broadcasted_iota(jnp.int32, (SUBL, LANES), 0)


def lane_iota():
    return lax.broadcasted_iota(jnp.int32, (SUBL, LANES), 1)


def keep_of(plan, wave_x, wave_y):
    return (3 * wave_x < plan["length"]) & (3 * jnp.abs(wave_y) < plan["length"])


def fetch_slots(slots, pairs, sems):
    j = pl.program_id(0)

    def copy(n, slot):
        source, held = pairs[n]
        return pltpu.make_async_copy(source.at[:, slot], held.at[slot], sems.at[n, slot])

    @pl.when(j == 0)
    def _():
        @pl.loop(0, slots)
        def _(slot):
            for n in range(len(pairs)):
                copy(n, slot).start()

    for n in range(len(pairs)):
        copy(n, j).wait()
    return j


def lines_in_kernel(plan, parity, lines, turn, wh, wl, out, psi, scr, held, sems):
    length = plan["length"]
    j = fetch_slots(plan["slots"], [(lines, held)], sems)
    half = HALF // 2
    wave_x = first_line(plan, pl.program_id(0)) + sublane_iota()
    kx = wave_x.astype(jnp.float32)
    kx_sq = kx * kx
    doubled = jnp.where(wave_x == 0, 1.0, 2.0) * (length / 9.0)
    step = wave_scale / length
    lane = lane_iota().astype(jnp.float32)
    keep_x = 3 * wave_x < length
    tiles = kept_tiles(plan)
    edges = (plan["low"] - 1, HALF - plan["low"])

    def ky_of(a):
        return lane + float(LANES * a - (length if a >= half else 0))

    for t, a in enumerate(tiles):
        off = tile_of(plan, a)
        ky = ky_of(a)
        factor = doubled / jnp.maximum(kx_sq + ky * ky, 1.0)
        keep = keep_x & (3.0 * jnp.abs(ky) < length) if a in edges else keep_x
        re, im = (jnp.where(keep, held[j, p, :, off:off + LANES], 0.0) for p in range(2))
        psi[t, 0] = -factor * im
        psi[t, 1] = factor * re
    for field in range(2):
        values = {}
        for t, a in enumerate(tiles):
            weight = step * ky_of(a) if field == 0 else -step * kx
            values[a] = (psi[t, 0] * weight, psi[t, 1] * weight)
        mixed = []
        for a in range(half):
            x0, x1 = values.get(a), values.get(a + half)
            if parity == 0:
                mixed.append(cadd(x0, x1))
            else:
                mixed.append(cturn(csub(x0, x1), a, HALF, 1))
        result = butterflies(mixed, 1, range(half))
        for e in range(half):
            re, im = result[e]
            cosine, sine_part = turn[e, 0:1, :], turn[e, 1:2, :]
            first = (field * half + e) * SUBL
            at = slice(first, first + SUBL)
            scr[at, 0:LANES] = re * cosine - im * sine_part
            scr[at, LANES:] = re * sine_part + im * cosine
    spread = dot3(halves(scr[...]), (wh[...], wl[...]))
    for field in range(2):
        rows = spread[field * half * SUBL:(field + 1) * half * SUBL]
        for s in range(2):
            out[:, 0, field, s] = rows[:, s * LANES:(s + 1) * LANES].reshape(half, SUBL, LANES)


def lines_in(plan, parity, lines, turn, table):
    slots = plan["slots"]
    width = 2 * plan["low"] * LANES
    devices = plan["rows"] * plan["cols"]
    whole = lambda shape: pl.BlockSpec(shape, lambda j: (0,) * len(shape))
    return pl.pallas_call(
        functools.partial(lines_in_kernel, plan, parity),
        grid=(slots,),
        in_specs=[
            pl.BlockSpec(memory_space=pl.ANY),
            whole((HALF // 2, 2, LANES)),
            whole((2 * LANES, 2 * LANES)),
            whole((2 * LANES, 2 * LANES)),
        ],
        out_specs=pl.BlockSpec((devices, 1, 2, 2, SUBL, LANES), lambda j: (0, j, 0, 0, 0, 0)),
        out_shape=jax.ShapeDtypeStruct((devices, slots, 2, 2, SUBL, LANES), jnp.float32),
        scratch_shapes=[
            pltpu.VMEM((2 * plan["low"], 2, SUBL, LANES), jnp.float32),
            pltpu.VMEM((HALF * SUBL, 2 * LANES), jnp.float32),
            pltpu.VMEM((slots, 2, SUBL, width), jnp.float32),
            pltpu.SemaphoreType.DMA((1, slots)),
        ],
        compiler_params=pltpu.CompilerParams(vmem_limit_bytes=60 << 20),
        cost_estimate=pl.CostEstimate(flops=4 << 30, bytes_accessed=16 << 20, transcendentals=0),
        name="lines_in",
    )(lines, turn, *table)


def columns_kernel(plan, src, th, tl, fh, fl, out, mid):
    rows = plan["rows"]
    low = plan["low"]
    per_tile = LANES // SUBL
    quarter = per_tile // rows
    inside = [[home_of(plan, a * per_tile + q * rows) for a in range(low)] for q in range(quarter)]
    used = {place for line in inside for place in line if place}

    @pl.loop(0, 2 * rows)
    def _(i):
        r = i % rows
        field = i // rows
        lanes = pl.ds(pl.multiple_of(field * LANES, LANES), LANES)
        for q in range(quarter):
            values = []
            for a in range(HALF):
                place = inside[q][a] if a < low else None
                if place is None:
                    values.append(None)
                    continue
                at = (place[0] * rows + r, place[1], field)
                values.append((src[at + (0,)], src[at + (1,)]))
            result = butterflies(values, 1, range(HALF))
            base = pl.multiple_of((q * rows + r) * SUBL, SUBL)
            for c in range(HALF):
                mid[c, pl.ds(base, SUBL), lanes] = result[c][0]
                mid[c, pl.ds(LANES + base, SUBL), lanes] = result[c][1]

    @pl.loop(0, HALF)
    def _(c):
        grid = dot3((th[c], tl[c]), halves(mid[c]))
        u, v = grid[:, :LANES], grid[:, LANES:]
        pair = jnp.concatenate([u * v, (v - u) * (v + u)], axis=1)
        mid[c] = dot3((fh[c], fl[c]), halves(pair))

    @pl.loop(0, 2 * rows)
    def _(i):
        r = i % rows
        field = i // rows
        lanes = pl.ds(pl.multiple_of(field * LANES, LANES), LANES)
        for q in range(quarter):
            base = pl.multiple_of((q * rows + r) * SUBL, SUBL)
            values = [
                (mid[c, pl.ds(base, SUBL), lanes], mid[c, pl.ds(LANES + base, SUBL), lanes])
                for c in range(HALF)
            ]
            need = [a for a in range(low) if inside[q][a]]
            result = butterflies(values, -1, need)
            for a in need:
                place = inside[q][a]
                at = (place[0] * rows + r, place[1], field)
                out[at + (0,)] = result[a][0]
                out[at + (1,)] = result[a][1]
        for col in range(plan["cols"]):
            for slot in range(plan["slots"]):
                if (col, slot) not in used:
                    for p in range(2):
                        out[col * rows + r, slot, field, p] = jnp.zeros(
                            (SUBL, LANES), jnp.float32
                        )


def columns(plan, spread, tables):
    return pl.pallas_call(
        functools.partial(columns_kernel, plan),
        in_specs=[pl.BlockSpec(memory_space=pltpu.VMEM)] * 5,
        out_specs=pl.BlockSpec(memory_space=pltpu.VMEM),
        out_shape=jax.ShapeDtypeStruct(spread.shape, jnp.float32),
        scratch_shapes=[pltpu.VMEM((HALF, 2 * LANES, 2 * LANES), jnp.float32)],
        compiler_params=pltpu.CompilerParams(vmem_limit_bytes=60 << 20),
        cost_estimate=pl.CostEstimate(flops=16 << 30, bytes_accessed=30 << 20, transcendentals=0),
        name="columns",
    )(spread, *tables)


def lines_out_kernel(plan, got0, got1, turn, wh, wl, lines, scr, acc, held0, held1, sems):
    length = plan["length"]
    j = fetch_slots(plan["slots"], [(got0, held0), (got1, held1)], sems)
    half = HALF // 2
    wave_x = first_line(plan, pl.program_id(0)) + sublane_iota()
    step = wave_scale / length
    kappa_x = step * wave_x.astype(jnp.float32)
    kappa_x_sq = kappa_x * kappa_x
    lane = lane_iota().astype(jnp.float32)
    keep_x = 3 * wave_x < length
    tiles = kept_tiles(plan)
    edges = (plan["low"] - 1, HALF - plan["low"])
    rows = half * SUBL
    both = jnp.concatenate(
        [
            jnp.concatenate([held[j, :, field, s].reshape(rows, LANES) for s in range(2)], axis=1)
            for field in range(2) for held in (held0, held1)
        ],
        axis=0,
    )
    scr[...] = dot3(halves(both), (wh[...], wl[...]))
    for field in range(2):
        values = []
        for c in range(HALF):
            e, parity = c // 2, c % 2
            first = ((2 * field + parity) * half + e) * SUBL
            at = slice(first, first + SUBL)
            re, im = scr[at, 0:LANES], scr[at, LANES:]
            cosine, sine_part = turn[parity, e, 0:1, :], turn[parity, e, 1:2, :]
            values.append((re * cosine + im * sine_part, im * cosine - re * sine_part))
        result = butterflies(values, -1, tiles)
        for t, a in enumerate(tiles):
            ky = lane + float(LANES * a - (length if a >= half else 0))
            kappa_y = step * ky
            if field == 0:
                weight = (kappa_x_sq - kappa_y * kappa_y) * (1.0 / length)
            else:
                weight = kappa_x * kappa_y * (1.0 / length)
            keep = keep_x & (3.0 * jnp.abs(ky) < length) if a in edges else keep_x
            off = tile_of(plan, a)
            for p in range(2):
                value = weight * result[a][p]
                if field == 0:
                    acc[t, p] = value
                else:
                    lines[p, 0, :, off:off + LANES] = jnp.where(keep, acc[t, p] + value, 0.0)


def lines_out(plan, got0, got1, turn, table):
    slots = plan["slots"]
    width = 2 * plan["low"] * LANES
    devices = plan["rows"] * plan["cols"]
    whole = lambda shape: pl.BlockSpec(shape, lambda j: (0,) * len(shape))
    got_spec = pl.BlockSpec(memory_space=pl.ANY)
    return pl.pallas_call(
        functools.partial(lines_out_kernel, plan),
        grid=(slots,),
        in_specs=[
            got_spec,
            got_spec,
            whole((2, HALF // 2, 2, LANES)),
            whole((2 * LANES, 2 * LANES)),
            whole((2 * LANES, 2 * LANES)),
        ],
        out_specs=pl.BlockSpec((2, 1, SUBL, width), lambda j: (0, j, 0, 0)),
        out_shape=jax.ShapeDtypeStruct((2, slots, SUBL, width), jnp.float32),
        scratch_shapes=[
            pltpu.VMEM((2 * HALF * SUBL, 2 * LANES), jnp.float32),
            pltpu.VMEM((2 * plan["low"], 2, SUBL, LANES), jnp.float32),
            pltpu.VMEM((slots, devices, 2, 2, SUBL, LANES), jnp.float32),
            pltpu.VMEM((slots, devices, 2, 2, SUBL, LANES), jnp.float32),
            pltpu.SemaphoreType.DMA((2, slots)),
        ],
        compiler_params=pltpu.CompilerParams(vmem_limit_bytes=60 << 20),
        cost_estimate=pl.CostEstimate(flops=8 << 30, bytes_accessed=22 << 20, transcendentals=0),
        name="lines_out",
    )(got0, got1, turn, *table)


def spans(plan, row):
    full = plan["block_y"]
    short = plan["low"] * LANES - full
    side, inner = row // 2, row % 2

    def at(offset):
        return pl.multiple_of(offset, LANES)

    return (
        (at(side * (full - short)), at(side * (full + short) + inner * full), short),
        (at((1 - side) * short), at(short + side * (full + short)), full - short),
    )


def both_of(row):
    return row // 2 == row % 2


def own_cases(plan):
    cases = []
    for col, count in enumerate(plan["own"]):
        count = min(count, plan["slots"])
        if not count:
            continue
        if cases and cases[-1][2] == count:
            cases[-1] = (cases[-1][0], col, count)
        else:
            cases.append((col, col, count))
    return cases


def exchange_kernel(plan, back, source, target, send, recv):
    rows, slots, extra = plan["rows"], plan["slots"], plan["extra"]
    row, col = lax.axis_index("row"), lax.axis_index("col")

    def views(home, lines, begin, count, start, line_row, home_row, piece):
        home_at, line_at, width = spans(plan, home_row)[piece]
        return (
            home.at[:, pl.ds(begin, count), line_row, :, pl.ds(home_at, width)],
            lines.at[:, pl.ds(start, count), :, pl.ds(line_at, width)],
        )

    def copy(kind, step, piece, begin, count, start, where, line_row, home_row, turn):
        if back:
            dst, src = views(target, source, begin, count, start, line_row, home_row, piece)
        else:
            src, dst = views(source, target, begin, count, start, line_row, home_row, piece)
        if where is None:
            return pltpu.make_async_copy(src, dst, send.at[kind, step, piece])
        return pltpu.make_async_remote_copy(
            src_ref=src, dst_ref=dst, send_sem=send.at[kind + turn, step, piece],
            recv_sem=recv.at[kind + turn, step, piece], device_id=where,
            device_id_type=pl.DeviceIdType.MESH,
        )

    def each(home_row, act):
        act(0)

        @pl.when(both_of(home_row))
        def _():
            act(1)

    def moved(verb):
        for donor, taker, turn in plan["moves"]:
            start = slots - extra if turn == 0 else 0
            sender, receiver = (taker, donor) if back else (donor, taker)
            peer = sender if verb == "recv" else receiver

            @pl.when(col == (receiver if verb == "recv" else sender))
            def _():
                for step in range(rows):
                    other = (row + step) % rows if verb != "recv" else (row + rows - step) % rows
                    mine_is_line = back == (verb != "recv")
                    line_row, home_row = (row, other) if mine_is_line else (other, row)

                    def act(piece):
                        it = copy(
                            1, step, piece, slots, extra, start,
                            {"col": peer, "row": other}, line_row, home_row, turn,
                        )
                        do(it, verb)

                    each(home_row, act)

    def do(it, verb):
        if verb == "start":
            it.start()
        elif verb == "send":
            it.wait_send()
        else:
            it.wait_recv()

    def owned(verb):
        for first, last, count in own_cases(plan):
            @pl.when((col >= first) & (col <= last))
            def _():
                for step in range(1, rows):
                    other = (row + step) % rows if verb != "recv" else (row + rows - step) % rows
                    mine_is_line = back == (verb != "recv")
                    line_row, home_row = (row, other) if mine_is_line else (other, row)

                    def act(piece):
                        do(
                            copy(
                                0, step, piece, 0, count, 0, {"row": other}, line_row,
                                home_row, 0,
                            ),
                            verb,
                        )

                    each(home_row, act)

    def local(verb):
        for first, last, count in own_cases(plan):
            @pl.when((col >= first) & (col <= last))
            def _():
                def act(piece):
                    it = copy(0, 0, piece, 0, count, 0, None, row, row, 0)
                    if verb == "start":
                        it.start()
                    else:
                        it.wait()

                each(row, act)

    moved("start")
    owned("start")
    local("start")
    local("wait")
    owned("recv")
    moved("recv")
    owned("send")
    moved("send")


def exchange(plan, back, source):
    rows, groups = plan["rows"], plan["groups"]
    home = (2, groups, rows, SUBL, plan["block_y"])
    lines = (2, plan["slots"], SUBL, 2 * plan["low"] * LANES)
    turns_used = 3
    return pl.pallas_call(
        functools.partial(exchange_kernel, plan, back),
        in_specs=[pl.BlockSpec(memory_space=pl.ANY)],
        out_specs=pl.BlockSpec(memory_space=pl.ANY),
        out_shape=jax.ShapeDtypeStruct(home if back else lines, jnp.float32),
        scratch_shapes=[
            pltpu.SemaphoreType.DMA((turns_used, rows, 2)),
            pltpu.SemaphoreType.DMA((turns_used, rows, 2)),
        ],
        compiler_params=pltpu.CompilerParams(has_side_effects=True, vmem_limit_bytes=60 << 20),
        cost_estimate=pl.CostEstimate(flops=1 << 34, bytes_accessed=16 << 20, transcendentals=0),
        name="lines_home" if back else "home_lines",
    )(source)


def split_table(values):
    high = lax.reduce_precision(values, 8, 7)
    return high.astype(jnp.bfloat16), (values - high).astype(jnp.bfloat16)


def angle_pair(rows, cols, period):
    row_ids = lax.broadcasted_iota(jnp.int32, (rows, cols), 0)
    col_ids = lax.broadcasted_iota(jnp.int32, (rows, cols), 1)
    angles = 2.0 * math.pi / period * (row_ids * col_ids % period).astype(jnp.float32)
    return jnp.cos(angles), jnp.sin(angles)


def lane_table(sign):
    cosine, sine_part = angle_pair(LANES, LANES, LANES)
    sine_part = sign * sine_part
    return split_table(
        jnp.concatenate(
            [
                jnp.concatenate([cosine, sine_part], axis=1),
                jnp.concatenate([-sine_part, cosine], axis=1),
            ],
            axis=0,
        )
    )


def turns(length):
    cosine, sine_part = angle_pair(HALF, LANES, length)
    both = jnp.stack([cosine, sine_part], axis=1).reshape(HALF // 2, 2, 2, LANES)
    return jnp.swapaxes(both, 0, 1)


def column_tables(length):
    cos_b, sin_b = angle_pair(LANES, LANES, LANES)
    cos_c, sin_c = angle_pair(HALF, LANES, length)

    def both(turn_shape, axis):
        ct, st = cos_c.reshape(turn_shape), sin_c.reshape(turn_shape)
        cosine = ct * cos_b - st * sin_b
        sine_part = st * cos_b + ct * sin_b
        return split_table(jnp.concatenate([cosine, -sine_part], axis=axis))

    inverse = both((HALF, 1, LANES), 2)
    forward = both((HALF, LANES, 1), 1)
    return inverse + forward


def fast_term(plan, field):
    rows = plan["rows"]

    def across(lines):
        return lax.all_to_all(lines, ("col", "row"), split_axis=0, concat_axis=0, tiled=True)

    home = field.reshape(2, plan["groups"], rows, SUBL, plan["block_y"])
    lines = exchange(plan, False, home)
    turn = turns(plan["length"])
    table = lane_table(1.0)
    spread = [
        across(lines_in(plan, parity, lines, turn[parity], table)) for parity in range(2)
    ]
    tables = column_tables(plan["length"])
    back = [across(columns(plan, part, tables)) for part in spread]
    lines = lines_out(plan, *back, turn, lane_table(-1.0))
    return exchange(plan, True, lines).reshape(field.shape)


def fast_device(plan, start_field, section_field, start_term, first_term, second_term):
    wave_x, wave_y = positions(
        (plan["block_x"], plan["block_y"]),
        lax.axis_index("col") * plan["block_x"],
        lax.axis_index("row") * plan["block_y"],
        plan["length"],
    )
    damping, weight_a, weight_b, weight_c = section_weights(wave_x, wave_y, plan["length"])[:4]
    linear = (
        damping * start_field
        + weight_a * start_term
        + 2.0 * weight_b * (first_term + second_term)
    )
    linear, weight_c = lax.optimization_barrier((linear, weight_c))
    term = jnp.stack([fast_term(plan, section_field[m]) for m in range(start_field.shape[0])])
    keep = keep_of(plan, wave_x, wave_y)
    return linear + jnp.where(keep, weight_c * term, 0.0)


def solution(mesh):
    rows, cols = mesh.shape["row"], mesh.shape["col"]

    def body(start_field, *rest):
        block_x, block_y = start_field.shape[2], start_field.shape[3]
        plan = plan_of(block_y * rows, rows, cols, block_x, block_y)
        if plan is None:
            return per_device(start_field, *rest)
        return fast_device(plan, start_field, *rest)

    return jax.shard_map(
        body,
        mesh=mesh,
        in_specs=(P(None, None, "col", "row"),) * 5,
        out_specs=P(None, None, "col", "row"),
        check_vma=False,
    )
```

```python
import functools
import math

import jax
import jax.numpy as jnp
from jax import lax
from jax.experimental import pallas as pl
from jax.experimental.pallas import tpu as pltpu
from jax.sharding import PartitionSpec as P

RADIX = 128


viscous_rate = 1.5
wave_scale = 3.0
series_terms = 12


def section_weights(wave_x, wave_y, length):
    square = wave_x * wave_x + wave_y * wave_y
    kappa_x = wave_scale * wave_x.astype(jnp.float32) / length
    kappa_y = wave_scale * wave_y.astype(jnp.float32) / length
    kappa_sq = kappa_x * kappa_x + kappa_y * kappa_y
    zvalue = -viscous_rate * kappa_sq
    damping = jnp.exp(zvalue)
    near_zero = 27 * square < 2 * length * length

    def series(degree):
        running = jnp.full_like(zvalue, 1.0 / math.factorial(series_terms - 1 + degree))
        for term_index in range(series_terms - 2, -1, -1):
            running = running * zvalue + 1.0 / math.factorial(term_index + degree)
        return running

    clamped = jnp.where(near_zero, -1.0, zvalue)
    exp_clamped = jnp.exp(clamped)
    closed_one = (exp_clamped - 1.0) / clamped
    closed_two = (exp_clamped - 1.0 - clamped) / (clamped * clamped)
    closed_three = (exp_clamped - 1.0 - clamped - 0.5 * clamped * clamped) / (
        clamped * clamped * clamped
    )
    phi_one = jnp.where(near_zero, series(1), closed_one)
    phi_two = jnp.where(near_zero, series(2), closed_two)
    phi_three = jnp.where(near_zero, series(3), closed_three)
    weight_a = phi_one - 3.0 * phi_two + 4.0 * phi_three
    weight_b = phi_two - 2.0 * phi_three
    weight_c = 4.0 * phi_three - phi_two
    keep_mask = ((3 * jnp.abs(wave_x) < length) & (3 * jnp.abs(wave_y) < length)).astype(
        jnp.float32
    )
    inverse_sq = length * length / (9.0 * jnp.maximum(square, 1).astype(jnp.float32))
    return (damping, weight_a, weight_b, weight_c, kappa_x, kappa_y, keep_mask, inverse_sq)


def section_table(count_in, count_out, period, direction):
    row_ids = lax.broadcasted_iota(jnp.int32, (count_in, count_out), 0)
    col_ids = lax.broadcasted_iota(jnp.int32, (count_in, count_out), 1)
    angles = direction * 2.0 * math.pi / period * (row_ids * col_ids % period).astype(jnp.float32)
    cosine = jnp.cos(angles)
    sine_part = jnp.sin(angles)
    return jnp.stack(
        [jnp.stack([cosine, sine_part], axis=1), jnp.stack([-sine_part, cosine], axis=1)], axis=0
    )


def twiddle(count_c, count_b, period, direction):
    row_ids = lax.broadcasted_iota(jnp.int32, (count_c, count_b), 0)
    col_ids = lax.broadcasted_iota(jnp.int32, (count_c, count_b), 1)
    angles = direction * 2.0 * math.pi / period * (row_ids * col_ids % period).astype(jnp.float32)
    return (jnp.cos(angles), jnp.sin(angles))


def rotate(values, cosine, sine_part):
    return jnp.stack(
        [values[0] * cosine - values[1] * sine_part, values[0] * sine_part + values[1] * cosine]
    )


def product(equation, left, right):
    return jnp.einsum(equation, left, right, precision=lax.Precision.HIGH)


def lines_inverse(pieces):
    parts, count_k, length = pieces.shape
    count_b = RADIX
    count_a = length // count_b
    shaped = pieces.reshape((parts, count_k, count_a, count_b))
    first = product("pkab,pasc->skcb", shaped, section_table(count_a, count_a, count_a, 1.0))
    first = rotate(first, *twiddle(count_a, count_b, length, 1.0))
    second = product("pkcb,pbsd->skcd", first, section_table(count_b, count_b, count_b, 1.0))
    return second.reshape((parts, count_k, length))


def lines_forward(pieces):
    parts, count_k, length = pieces.shape
    count_d = RADIX
    count_c = length // count_d
    shaped = pieces.reshape((parts, count_k, count_c, count_d))
    first = product("pkcd,pdsf->skcf", shaped, section_table(count_d, count_d, count_d, -1.0))
    first = rotate(first, *twiddle(count_c, count_d, length, -1.0))
    second = product("pkcf,pcse->skef", first, section_table(count_c, count_c, count_c, -1.0))
    return second.reshape((parts, count_k, length))


def turned_table(count_c, count_b, period, direction):
    c_ids = lax.broadcasted_iota(jnp.int32, (count_c, count_b, count_b), 0)
    b_ids = lax.broadcasted_iota(jnp.int32, (count_c, count_b, count_b), 1)
    d_ids = lax.broadcasted_iota(jnp.int32, (count_c, count_b, count_b), 2)
    steps = b_ids * (c_ids + count_c * d_ids) % period
    angles = direction * 2.0 * math.pi / period * steps.astype(jnp.float32)
    return jnp.cos(angles), jnp.sin(angles)


def columns_inverse(pieces, table):
    parts, half_count, count_y = pieces.shape
    count_a = half_count // RADIX
    count_c = 2 * count_a
    shaped = pieces.reshape((parts, count_a, RADIX, count_y))
    first = product("paby,pasc->csby", shaped, section_table(count_a, count_c, count_c, 1.0))
    return product("csby,csbd->cdy", first, table)


def columns_forward(grid, table):
    count_c, count_d, count_y = grid.shape
    half_count = count_c // 2
    first = product("cdy,cpfd->cpfy", grid, table)
    second = product(
        "cpfy,pcse->sefy", first, section_table(count_c, half_count, count_c, -1.0)
    )
    return second.reshape((2, half_count * count_d, count_y))


def to_columns(lines):
    return lax.all_to_all(lines, ("col", "row"), split_axis=2, concat_axis=1, tiled=True)


def to_lines(columns):
    return lax.all_to_all(columns, ("col", "row"), split_axis=1, concat_axis=2, tiled=True)


def positions(shape, start_x, start_y, length):
    wave_x = start_x + lax.broadcasted_iota(jnp.int32, shape, 0)
    index_y = start_y + lax.broadcasted_iota(jnp.int32, shape, 1)
    wave_y = jnp.where(index_y < length // 2, index_y, index_y - length)
    return wave_x, wave_y


def nonlinear(section_field, length):
    block_x = section_field.shape[1]
    lines = lax.all_to_all(section_field, "row", split_axis=1, concat_axis=2, tiled=True)
    count_k = lines.shape[1]
    start_x = lax.axis_index("col") * block_x + lax.axis_index("row") * count_k
    wave_x, wave_y = positions((count_k, length), start_x, 0, length)
    square = wave_x * wave_x + wave_y * wave_y
    kappa_x = wave_scale * wave_x.astype(jnp.float32) / length
    kappa_y = wave_scale * wave_y.astype(jnp.float32) / length
    keep = (3 * jnp.abs(wave_x) < length) & (3 * jnp.abs(wave_y) < length)
    doubled = jnp.where(wave_x == 0, 1.0, 2.0) * (1.0 / length)
    inverse_sq = length * length / (9.0 * jnp.maximum(square, 1).astype(jnp.float32))
    factor = jnp.where(keep, inverse_sq * doubled, 0.0)
    scale_u = kappa_y * factor
    scale_v = kappa_x * factor
    spec_u = jnp.stack([-scale_u * lines[1], scale_u * lines[0]])
    spec_v = jnp.stack([scale_v * lines[1], -scale_v * lines[0]])
    count_c = length // RADIX
    cosine, sine_part = turned_table(count_c, RADIX, length, 1.0)
    table = jnp.stack([cosine, -sine_part], axis=1)
    vel_u = columns_inverse(to_columns(lines_inverse(spec_u)), table)
    vel_v = columns_inverse(to_columns(lines_inverse(spec_v)), table)
    cross = lines_forward(to_lines(columns_forward(vel_u * vel_v, table)))
    square_gap = lines_forward(
        to_lines(columns_forward((vel_v - vel_u) * (vel_v + vel_u), table))
    )
    scale = jnp.where(keep, 1.0 / length, 0.0)
    weight_cross = (kappa_x * kappa_x - kappa_y * kappa_y) * scale
    weight_gap = kappa_x * kappa_y * scale
    term = weight_cross * cross + weight_gap * square_gap
    return lax.all_to_all(term, "row", split_axis=2, concat_axis=1, tiled=True)


def per_device(start_field, section_field, start_term, first_term, second_term):
    members = start_field.shape[0]
    block_x = start_field.shape[2]
    block_y = start_field.shape[3]
    length = block_y * lax.axis_size("row")
    wave_x, wave_y = positions(
        (block_x, block_y),
        lax.axis_index("col") * block_x,
        lax.axis_index("row") * block_y,
        length,
    )
    damping, weight_a, weight_b, weight_c = section_weights(wave_x, wave_y, length)[:4]
    linear = (
        damping * start_field
        + weight_a * start_term
        + 2.0 * weight_b * (first_term + second_term)
    )
    linear, weight_c = lax.optimization_barrier((linear, weight_c))
    section_term = jnp.stack([nonlinear(section_field[m], length) for m in range(members)])
    return linear + weight_c * section_term


LANES = 128
SUBL = 8
HALF = 64


def plan_of(length, rows, cols, block_x, block_y):
    if length != LANES * HALF or rows != 4 or block_x % (rows * SUBL) or block_y * rows != length:
        return None
    kept = (length - 1) // 3 + 1
    stride = rows * SUBL
    groups = block_x // stride
    own = [min(groups, max(0, -(-(kept - c * block_x) // stride))) for c in range(cols)]
    slots = -(-sum(own) // cols)
    extra = groups - slots
    donors = [c for c in range(cols) if own[c] == groups]
    if extra <= 0 or 2 * extra > slots or any(slots < own[c] < groups for c in range(cols)):
        return None
    takers = [c for c in range(cols) if own[c] + extra <= slots]
    first = [(c, 0) for c in takers]
    second = [(c, 1) for c in takers if own[c] == 0]
    places = first + second
    if len(donors) > len(places):
        return None
    order = donors[-1:] + donors[:-1]
    moves = [(donor, taker, turn) for donor, (taker, turn) in zip(order, places)]
    low = (kept + LANES - 1) // LANES
    high = HALF - (length - kept + 1) // LANES
    if low != high or low % 2 or low > HALF // 2:
        return None
    if not block_y < low * LANES < 2 * block_y or block_y % LANES:
        return None
    return dict(
        kept=kept, stride=stride, groups=groups, own=own, slots=slots, extra=extra,
        moves=moves, low=low, rows=rows, cols=cols,
        block_x=block_x, block_y=block_y, length=length,
    )


def home_of(plan, group):
    per_block = plan["block_x"] // SUBL
    if group * SUBL >= plan["kept"]:
        return None
    col, inside = divmod(group, per_block)
    slot = inside // plan["rows"]
    if slot < plan["slots"]:
        return col, slot
    for donor, taker, turn in plan["moves"]:
        if donor == col:
            start = plan["slots"] - plan["extra"] if turn == 0 else 0
            return taker, start + slot - plan["slots"]
    raise ValueError("no place")


def first_line(plan, slot):
    slots, extra = plan["slots"], plan["extra"]
    col = lax.axis_index("col")
    base = col * plan["block_x"] + slot * plan["stride"]
    for donor, taker, turn in plan["moves"]:
        start = slots - extra if turn == 0 else 0
        moved = donor * plan["block_x"] + (slots + slot - start) * plan["stride"]
        here = (col == taker) & (slot >= start) & (slot < start + extra)
        base = jnp.where(here, moved, base)
    return base + lax.axis_index("row") * SUBL


def cadd(a, b):
    if a is None:
        return b
    if b is None:
        return a
    return (a[0] + b[0], a[1] + b[1])


def csub(a, b):
    if b is None:
        return a
    if a is None:
        return (-b[0], -b[1])
    return (a[0] - b[0], a[1] - b[1])


def cturn(a, step, period, sign):
    if a is None:
        return None
    step = step * sign % period
    if step == 0:
        return a
    if 4 * step == period:
        return (-a[1], a[0])
    if 2 * step == period:
        return (-a[0], -a[1])
    if 4 * step == 3 * period:
        return (a[1], -a[0])
    angle = 2.0 * math.pi * step / period
    cosine, sine_part = math.cos(angle), math.sin(angle)
    if 8 * step % period == 0:
        size = math.sqrt(0.5)
        sign_c, sign_s = (1 if cosine > 0 else -1), (1 if sine_part > 0 else -1)
        real = a[0] - a[1] if sign_c == sign_s else a[0] + a[1]
        imag = a[0] + a[1] if sign_c == sign_s else a[1] - a[0]
        return (real * (sign_c * size), imag * (sign_c * size))
    return (a[0] * cosine - a[1] * sine_part, a[0] * sine_part + a[1] * cosine)


def butterflies(values, sign, need):
    count = len(values)
    if all(v is None for v in values):
        return {k: None for k in need}
    if count == 1:
        return {k: values[0] for k in need}
    half = count // 2
    sub = sorted({k % half for k in need})
    even = butterflies(values[0::2], sign, sub)
    odd = butterflies(values[1::2], sign, sub)
    wanted = set(need)
    out = {}
    for k in sub:
        turned = cturn(odd[k], k, count, sign)
        if k in wanted:
            out[k] = cadd(even[k], turned)
        if k + half in wanted:
            out[k + half] = csub(even[k], turned)
    return out


def halves(values):
    high = values.astype(jnp.bfloat16)
    return high, (values - high.astype(jnp.float32)).astype(jnp.bfloat16)


def dot3(left, right):
    lh, ll = left
    rh, rl = right
    def mm(a, b):
        return jnp.dot(a, b, preferred_element_type=jnp.float32)
    return mm(lh, rh) + (mm(ll, rh) + mm(lh, rl))


def tile_of(plan, a):
    low = plan["low"]
    return LANES * (a if a < low else a - (HALF - 2 * low))


def kept_tiles(plan):
    low = plan["low"]
    return list(range(low)) + list(range(HALF - low, HALF))


def sublane_iota():
    return lax.broadcasted_iota(jnp.int32, (SUBL, LANES), 0)


def lane_iota():
    return lax.broadcasted_iota(jnp.int32, (SUBL, LANES), 1)


def keep_of(plan, wave_x, wave_y):
    return (3 * wave_x < plan["length"]) & (3 * jnp.abs(wave_y) < plan["length"])


def fetch_slots(slots, pairs, sems):
    j = pl.program_id(0)

    def copy(n, slot):
        source, held = pairs[n]
        return pltpu.make_async_copy(source.at[:, slot], held.at[slot], sems.at[n, slot])

    @pl.when(j == 0)
    def _():
        @pl.loop(0, slots)
        def _(slot):
            for n in range(len(pairs)):
                copy(n, slot).start()

    for n in range(len(pairs)):
        copy(n, j).wait()
    return j


def lines_in_kernel(plan, parity, lines, turn, wh, wl, out, psi, scr, held, sems):
    length = plan["length"]
    j = fetch_slots(plan["slots"], [(lines, held)], sems)
    half = HALF // 2
    wave_x = first_line(plan, pl.program_id(0)) + sublane_iota()
    kx = wave_x.astype(jnp.float32)
    kx_sq = kx * kx
    doubled = jnp.where(wave_x == 0, 1.0, 2.0) * (length / 9.0)
    step = wave_scale / length
    lane = lane_iota().astype(jnp.float32)
    keep_x = 3 * wave_x < length
    tiles = kept_tiles(plan)
    edges = (plan["low"] - 1, HALF - plan["low"])

    def ky_of(a):
        return lane + float(LANES * a - (length if a >= half else 0))

    for t, a in enumerate(tiles):
        off = tile_of(plan, a)
        ky = ky_of(a)
        factor = doubled / jnp.maximum(kx_sq + ky * ky, 1.0)
        keep = keep_x & (3.0 * jnp.abs(ky) < length) if a in edges else keep_x
        re, im = (jnp.where(keep, held[j, p, :, off:off + LANES], 0.0) for p in range(2))
        psi[t, 0] = -factor * im
        psi[t, 1] = factor * re
    for field in range(2):
        values = {}
        for t, a in enumerate(tiles):
            weight = step * ky_of(a) if field == 0 else -step * kx
            values[a] = (psi[t, 0] * weight, psi[t, 1] * weight)
        mixed = []
        for a in range(half):
            x0, x1 = values.get(a), values.get(a + half)
            if parity == 0:
                mixed.append(cadd(x0, x1))
            else:
                mixed.append(cturn(csub(x0, x1), a, HALF, 1))
        result = butterflies(mixed, 1, range(half))
        for e in range(half):
            re, im = result[e]
            cosine, sine_part = turn[e, 0:1, :], turn[e, 1:2, :]
            first = (field * half + e) * SUBL
            at = slice(first, first + SUBL)
            scr[at, 0:LANES] = re * cosine - im * sine_part
            scr[at, LANES:] = re * sine_part + im * cosine
    spread = dot3(halves(scr[...]), (wh[...], wl[...]))
    for field in range(2):
        rows = spread[field * half * SUBL:(field + 1) * half * SUBL]
        for s in range(2):
            out[:, 0, field, s] = rows[:, s * LANES:(s + 1) * LANES].reshape(half, SUBL, LANES)


def lines_in(plan, parity, lines, turn, table):
    slots = plan["slots"]
    width = 2 * plan["low"] * LANES
    devices = plan["rows"] * plan["cols"]
    whole = lambda shape: pl.BlockSpec(shape, lambda j: (0,) * len(shape))
    return pl.pallas_call(
        functools.partial(lines_in_kernel, plan, parity),
        grid=(slots,),
        in_specs=[
            pl.BlockSpec(memory_space=pl.ANY),
            whole((HALF // 2, 2, LANES)),
            whole((2 * LANES, 2 * LANES)),
            whole((2 * LANES, 2 * LANES)),
        ],
        out_specs=pl.BlockSpec((devices, 1, 2, 2, SUBL, LANES), lambda j: (0, j, 0, 0, 0, 0)),
        out_shape=jax.ShapeDtypeStruct((devices, slots, 2, 2, SUBL, LANES), jnp.float32),
        scratch_shapes=[
            pltpu.VMEM((2 * plan["low"], 2, SUBL, LANES), jnp.float32),
            pltpu.VMEM((HALF * SUBL, 2 * LANES), jnp.float32),
            pltpu.VMEM((slots, 2, SUBL, width), jnp.float32),
            pltpu.SemaphoreType.DMA((1, slots)),
        ],
        compiler_params=pltpu.CompilerParams(vmem_limit_bytes=60 << 20),
        cost_estimate=pl.CostEstimate(flops=4 << 30, bytes_accessed=16 << 20, transcendentals=0),
        name="lines_in",
    )(lines, turn, *table)


def columns_kernel(plan, src, th, tl, fh, fl, out, mid):
    rows = plan["rows"]
    low = plan["low"]
    per_tile = LANES // SUBL
    quarter = per_tile // rows
    inside = [[home_of(plan, a * per_tile + q * rows) for a in range(low)] for q in range(quarter)]
    used = {place for line in inside for place in line if place}

    @pl.loop(0, 2 * rows)
    def _(i):
        r = i % rows
        field = i // rows
        lanes = pl.ds(pl.multiple_of(field * LANES, LANES), LANES)
        for q in range(quarter):
            values = []
            for a in range(HALF):
                place = inside[q][a] if a < low else None
                if place is None:
                    values.append(None)
                    continue
                at = (place[0] * rows + r, place[1], field)
                values.append((src[at + (0,)], src[at + (1,)]))
            result = butterflies(values, 1, range(HALF))
            base = pl.multiple_of((q * rows + r) * SUBL, SUBL)
            for c in range(HALF):
                mid[c, pl.ds(base, SUBL), lanes] = result[c][0]
                mid[c, pl.ds(LANES + base, SUBL), lanes] = result[c][1]

    @pl.loop(0, HALF)
    def _(c):
        grid = dot3((th[c], tl[c]), halves(mid[c]))
        u, v = grid[:, :LANES], grid[:, LANES:]
        pair = jnp.concatenate([u * v, (v - u) * (v + u)], axis=1)
        mid[c] = dot3((fh[c], fl[c]), halves(pair))

    @pl.loop(0, 2 * rows)
    def _(i):
        r = i % rows
        field = i // rows
        lanes = pl.ds(pl.multiple_of(field * LANES, LANES), LANES)
        for q in range(quarter):
            base = pl.multiple_of((q * rows + r) * SUBL, SUBL)
            values = [
                (mid[c, pl.ds(base, SUBL), lanes], mid[c, pl.ds(LANES + base, SUBL), lanes])
                for c in range(HALF)
            ]
            need = [a for a in range(low) if inside[q][a]]
            result = butterflies(values, -1, need)
            for a in need:
                place = inside[q][a]
                at = (place[0] * rows + r, place[1], field)
                out[at + (0,)] = result[a][0]
                out[at + (1,)] = result[a][1]
        for col in range(plan["cols"]):
            for slot in range(plan["slots"]):
                if (col, slot) not in used:
                    for p in range(2):
                        out[col * rows + r, slot, field, p] = jnp.zeros(
                            (SUBL, LANES), jnp.float32
                        )


def columns(plan, spread, tables):
    return pl.pallas_call(
        functools.partial(columns_kernel, plan),
        in_specs=[pl.BlockSpec(memory_space=pltpu.VMEM)] * 5,
        out_specs=pl.BlockSpec(memory_space=pltpu.VMEM),
        out_shape=jax.ShapeDtypeStruct(spread.shape, jnp.float32),
        scratch_shapes=[pltpu.VMEM((HALF, 2 * LANES, 2 * LANES), jnp.float32)],
        compiler_params=pltpu.CompilerParams(vmem_limit_bytes=60 << 20),
        cost_estimate=pl.CostEstimate(flops=16 << 30, bytes_accessed=30 << 20, transcendentals=0),
        name="columns",
    )(spread, *tables)


def slot_out(plan, j, held0, held1, turn, wh, wl, lines, scr, acc):
    length = plan["length"]
    half = HALF // 2
    wave_x = first_line(plan, j) + sublane_iota()
    step = wave_scale / length
    kappa_x = step * wave_x.astype(jnp.float32)
    kappa_x_sq = kappa_x * kappa_x
    lane = lane_iota().astype(jnp.float32)
    keep_x = 3 * wave_x < length
    tiles = kept_tiles(plan)
    edges = (plan["low"] - 1, HALF - plan["low"])
    rows = half * SUBL
    both = jnp.concatenate(
        [
            jnp.concatenate([held[j, :, field, s].reshape(rows, LANES) for s in range(2)], axis=1)
            for field in range(2) for held in (held0, held1)
        ],
        axis=0,
    )
    scr[...] = dot3(halves(both), (wh[...], wl[...]))
    for field in range(2):
        values = []
        for c in range(HALF):
            e, parity = c // 2, c % 2
            first = ((2 * field + parity) * half + e) * SUBL
            at = slice(first, first + SUBL)
            re, im = scr[at, 0:LANES], scr[at, LANES:]
            cosine, sine_part = turn[parity, e, 0:1, :], turn[parity, e, 1:2, :]
            values.append((re * cosine + im * sine_part, im * cosine - re * sine_part))
        result = butterflies(values, -1, tiles)
        for t, a in enumerate(tiles):
            ky = lane + float(LANES * a - (length if a >= half else 0))
            kappa_y = step * ky
            if field == 0:
                weight = (kappa_x_sq - kappa_y * kappa_y) * (1.0 / length)
            else:
                weight = kappa_x * kappa_y * (1.0 / length)
            keep = keep_x & (3.0 * jnp.abs(ky) < length) if a in edges else keep_x
            off = tile_of(plan, a)
            for p in range(2):
                value = weight * result[a][p]
                if field == 0:
                    acc[t, p] = value
                else:
                    lines[j, p, :, off:off + LANES] = jnp.where(keep, acc[t, p] + value, 0.0)


def spans(plan, row):
    full = plan["block_y"]
    short = plan["low"] * LANES - full
    side, inner = row // 2, row % 2

    def at(offset):
        return pl.multiple_of(offset, LANES)

    return (
        (at(side * (full - short)), at(side * (full + short) + inner * full), short),
        (at((1 - side) * short), at(short + side * (full + short)), full - short),
    )


def both_of(row):
    return row // 2 == row % 2


def own_cases(plan):
    cases = []
    for col, count in enumerate(plan["own"]):
        count = min(count, plan["slots"])
        if not count:
            continue
        if cases and cases[-1][2] == count:
            cases[-1] = (cases[-1][0], col, count)
        else:
            cases.append((col, col, count))
    return cases


def exchange_kernel(plan, back, source, target, send, recv):
    rows, slots, extra = plan["rows"], plan["slots"], plan["extra"]
    row, col = lax.axis_index("row"), lax.axis_index("col")

    def views(home, lines, begin, count, start, line_row, home_row, piece):
        home_at, line_at, width = spans(plan, home_row)[piece]
        return (
            home.at[:, pl.ds(begin, count), line_row, :, pl.ds(home_at, width)],
            lines.at[:, pl.ds(start, count), :, pl.ds(line_at, width)],
        )

    def copy(kind, step, piece, begin, count, start, where, line_row, home_row, turn):
        if back:
            dst, src = views(target, source, begin, count, start, line_row, home_row, piece)
        else:
            src, dst = views(source, target, begin, count, start, line_row, home_row, piece)
        if where is None:
            return pltpu.make_async_copy(src, dst, send.at[kind, step, piece])
        return pltpu.make_async_remote_copy(
            src_ref=src, dst_ref=dst, send_sem=send.at[kind + turn, step, piece],
            recv_sem=recv.at[kind + turn, step, piece], device_id=where,
            device_id_type=pl.DeviceIdType.MESH,
        )

    def each(home_row, act):
        act(0)

        @pl.when(both_of(home_row))
        def _():
            act(1)

    def moved(verb):
        for donor, taker, turn in plan["moves"]:
            start = slots - extra if turn == 0 else 0
            sender, receiver = (taker, donor) if back else (donor, taker)
            peer = sender if verb == "recv" else receiver

            @pl.when(col == (receiver if verb == "recv" else sender))
            def _():
                for step in range(rows):
                    other = (row + step) % rows if verb != "recv" else (row + rows - step) % rows
                    mine_is_line = back == (verb != "recv")
                    line_row, home_row = (row, other) if mine_is_line else (other, row)

                    def act(piece):
                        it = copy(
                            1, step, piece, slots, extra, start,
                            {"col": peer, "row": other}, line_row, home_row, turn,
                        )
                        do(it, verb)

                    each(home_row, act)

    def do(it, verb):
        if verb == "start":
            it.start()
        elif verb == "send":
            it.wait_send()
        else:
            it.wait_recv()

    def owned(verb):
        for first, last, count in own_cases(plan):
            @pl.when((col >= first) & (col <= last))
            def _():
                for step in range(1, rows):
                    other = (row + step) % rows if verb != "recv" else (row + rows - step) % rows
                    mine_is_line = back == (verb != "recv")
                    line_row, home_row = (row, other) if mine_is_line else (other, row)

                    def act(piece):
                        do(
                            copy(
                                0, step, piece, 0, count, 0, {"row": other}, line_row,
                                home_row, 0,
                            ),
                            verb,
                        )

                    each(home_row, act)

    def local(verb):
        for first, last, count in own_cases(plan):
            @pl.when((col >= first) & (col <= last))
            def _():
                def act(piece):
                    it = copy(0, 0, piece, 0, count, 0, None, row, row, 0)
                    if verb == "start":
                        it.start()
                    else:
                        it.wait()

                each(row, act)

    moved("start")
    owned("start")
    local("start")
    local("wait")
    owned("recv")
    moved("recv")
    owned("send")
    moved("send")


def exchange(plan, back, source):
    rows, groups = plan["rows"], plan["groups"]
    home = (2, groups, rows, SUBL, plan["block_y"])
    lines = (2, plan["slots"], SUBL, 2 * plan["low"] * LANES)
    turns_used = 3
    return pl.pallas_call(
        functools.partial(exchange_kernel, plan, back),
        in_specs=[pl.BlockSpec(memory_space=pl.ANY)],
        out_specs=pl.BlockSpec(memory_space=pl.ANY),
        out_shape=jax.ShapeDtypeStruct(home if back else lines, jnp.float32),
        scratch_shapes=[
            pltpu.SemaphoreType.DMA((turns_used, rows, 2)),
            pltpu.SemaphoreType.DMA((turns_used, rows, 2)),
        ],
        compiler_params=pltpu.CompilerParams(has_side_effects=True, vmem_limit_bytes=60 << 20),
        cost_estimate=pl.CostEstimate(flops=1 << 34, bytes_accessed=16 << 20, transcendentals=0),
        name="lines_home" if back else "home_lines",
    )(source)


def lines_home_kernel(
    plan, got0, got1, turn, wh, wl, home, scr, acc, held0, held1, lines, sems, send, recv
):
    rows, slots, extra = plan["rows"], plan["slots"], plan["extra"]
    row, col = lax.axis_index("row"), lax.axis_index("col")
    pairs = ((got0, held0), (got1, held1))

    def fetch(n, slot):
        source, held = pairs[n]
        return pltpu.make_async_copy(source.at[:, slot], held.at[slot], sems.at[n, slot])

    def slot_of(i):
        return lax.rem(i + slots - extra, slots)

    def each(home_row, act):
        act(0)

        @pl.when(both_of(home_row))
        def _():
            act(1)

    def remote(source, target, kind, step, piece, where):
        return pltpu.make_async_remote_copy(
            src_ref=source, dst_ref=target, send_sem=send.at[kind, step, piece],
            recv_sem=recv.at[kind, step, piece], device_id=where,
            device_id_type=pl.DeviceIdType.MESH,
        )

    def put(slot, group, kind, where):
        for step in range(rows):
            other = (row + step) % rows

            def act(piece):
                home_at, line_at, width = spans(plan, other)[piece]
                source = lines.at[slot, :, :, pl.ds(line_at, width)]
                target = home.at[:, group, row, :, pl.ds(home_at, width)]
                if kind == 0 and step == 0:
                    pltpu.make_async_copy(source, target, send.at[0, 0, piece]).start()
                else:
                    remote(source, target, kind, step, piece, where(other)).start()

            each(other, act)

    def put_slot(slot):
        for donor, taker, turn_id in plan["moves"]:
            start = slots - extra if turn_id == 0 else 0

            @pl.when((col == taker) & (slot >= start) & (slot < start + extra))
            def _():
                put(
                    slot, slots + slot - start, 1 + turn_id,
                    lambda other: {"col": donor, "row": other},
                )

        for first, last, count in own_cases(plan):
            @pl.when((col >= first) & (col <= last) & (slot < count))
            def _():
                put(slot, slot, 0, lambda other: {"row": other})

    def block(begin, count, line_row, home_row, piece):
        home_at, _, width = spans(plan, home_row)[piece]
        return home.at[:, pl.ds(begin, count), line_row, :, pl.ds(home_at, width)]

    def settle(verb):
        def one(begin, count, kind, step, piece, where, line_row, home_row):
            at = block(begin, count, line_row, home_row, piece)
            if kind == 0 and step == 0:
                if verb == "send":
                    pltpu.make_async_copy(at, at, send.at[0, 0, piece]).wait()
                return
            it = remote(at, at, kind, step, piece, where)
            if verb == "send":
                it.wait_send()
            else:
                it.wait_recv()

        def all_of(begin, count, kind, where):
            for step in range(rows):
                if verb == "send":
                    other = (row + step) % rows
                    line_row, home_row = row, other
                else:
                    other = (row + rows - step) % rows
                    line_row, home_row = other, row
                each(
                    home_row,
                    lambda piece: one(
                        begin, count, kind, step, piece, where(other), line_row, home_row
                    ),
                )

        for first, last, count in own_cases(plan):
            @pl.when((col >= first) & (col <= last))
            def _():
                all_of(0, count, 0, lambda other: {"row": other})

        for donor, taker, turn_id in plan["moves"]:
            mine, peer = (taker, donor) if verb == "send" else (donor, taker)

            @pl.when(col == mine)
            def _():
                all_of(slots, extra, 1 + turn_id, lambda other: {"col": peer, "row": other})

    @pl.loop(0, slots)
    def _(i):
        for n in range(2):
            fetch(n, slot_of(i)).start()

    @pl.loop(0, slots)
    def _(i):
        slot = slot_of(i)
        for n in range(2):
            fetch(n, slot).wait()
        slot_out(plan, slot, held0, held1, turn, wh, wl, lines, scr, acc)

        @pl.when(i > 0)
        def _():
            put_slot(slot_of(i + slots - 1))

    put_slot(slot_of(slots - 1))
    settle("recv")
    settle("send")


def lines_home(plan, got0, got1, turn, table):
    slots, rows = plan["slots"], plan["rows"]
    width = 2 * plan["low"] * LANES
    devices = rows * plan["cols"]
    dma = pltpu.SemaphoreType.DMA
    held = pltpu.VMEM((slots, devices, 2, 2, SUBL, LANES), jnp.float32)
    return pl.pallas_call(
        functools.partial(lines_home_kernel, plan),
        in_specs=[pl.BlockSpec(memory_space=pl.ANY)] * 2
        + [pl.BlockSpec(memory_space=pltpu.VMEM)] * 3,
        out_specs=pl.BlockSpec(memory_space=pl.ANY),
        out_shape=jax.ShapeDtypeStruct(
            (2, plan["groups"], rows, SUBL, plan["block_y"]), jnp.float32
        ),
        scratch_shapes=[
            pltpu.VMEM((2 * HALF * SUBL, 2 * LANES), jnp.float32),
            pltpu.VMEM((2 * plan["low"], 2, SUBL, LANES), jnp.float32),
            held,
            held,
            pltpu.VMEM((slots, 2, SUBL, width), jnp.float32),
            dma((2, slots)),
            dma((3, rows, 2)),
            dma((3, rows, 2)),
        ],
        compiler_params=pltpu.CompilerParams(has_side_effects=True, vmem_limit_bytes=60 << 20),
        cost_estimate=pl.CostEstimate(flops=1 << 34, bytes_accessed=30 << 20, transcendentals=0),
        name="lines_home",
    )(got0, got1, turn, *table)


def split_table(values):
    high = lax.reduce_precision(values, 8, 7)
    return high.astype(jnp.bfloat16), (values - high).astype(jnp.bfloat16)


def angle_pair(rows, cols, period):
    row_ids = lax.broadcasted_iota(jnp.int32, (rows, cols), 0)
    col_ids = lax.broadcasted_iota(jnp.int32, (rows, cols), 1)
    angles = 2.0 * math.pi / period * (row_ids * col_ids % period).astype(jnp.float32)
    return jnp.cos(angles), jnp.sin(angles)


def lane_table(sign):
    cosine, sine_part = angle_pair(LANES, LANES, LANES)
    sine_part = sign * sine_part
    return split_table(
        jnp.concatenate(
            [
                jnp.concatenate([cosine, sine_part], axis=1),
                jnp.concatenate([-sine_part, cosine], axis=1),
            ],
            axis=0,
        )
    )


def turns(length):
    cosine, sine_part = angle_pair(HALF, LANES, length)
    both = jnp.stack([cosine, sine_part], axis=1).reshape(HALF // 2, 2, 2, LANES)
    return jnp.swapaxes(both, 0, 1)


def column_tables(length):
    cos_b, sin_b = angle_pair(LANES, LANES, LANES)
    cos_c, sin_c = angle_pair(HALF, LANES, length)

    def both(turn_shape, axis):
        ct, st = cos_c.reshape(turn_shape), sin_c.reshape(turn_shape)
        cosine = ct * cos_b - st * sin_b
        sine_part = st * cos_b + ct * sin_b
        return split_table(jnp.concatenate([cosine, -sine_part], axis=axis))

    inverse = both((HALF, 1, LANES), 2)
    forward = both((HALF, LANES, 1), 1)
    return inverse + forward


def fast_term(plan, field):
    rows = plan["rows"]

    def across(lines):
        return lax.all_to_all(lines, ("col", "row"), split_axis=0, concat_axis=0, tiled=True)

    home = field.reshape(2, plan["groups"], rows, SUBL, plan["block_y"])
    lines = exchange(plan, False, home)
    turn = turns(plan["length"])
    table = lane_table(1.0)
    spread = [
        across(lines_in(plan, parity, lines, turn[parity], table)) for parity in range(2)
    ]
    tables = column_tables(plan["length"])
    back = [across(columns(plan, part, tables)) for part in spread]
    return lines_home(plan, *back, turn, lane_table(-1.0)).reshape(field.shape)


def fast_device(plan, start_field, section_field, start_term, first_term, second_term):
    wave_x, wave_y = positions(
        (plan["block_x"], plan["block_y"]),
        lax.axis_index("col") * plan["block_x"],
        lax.axis_index("row") * plan["block_y"],
        plan["length"],
    )
    damping, weight_a, weight_b, weight_c = section_weights(wave_x, wave_y, plan["length"])[:4]
    linear = (
        damping * start_field
        + weight_a * start_term
        + 2.0 * weight_b * (first_term + second_term)
    )
    linear, weight_c = lax.optimization_barrier((linear, weight_c))
    term = jnp.stack([fast_term(plan, section_field[m]) for m in range(start_field.shape[0])])
    keep = keep_of(plan, wave_x, wave_y)
    return linear + jnp.where(keep, weight_c * term, 0.0)


def solution(mesh):
    rows, cols = mesh.shape["row"], mesh.shape["col"]

    def body(start_field, *rest):
        block_x, block_y = start_field.shape[2], start_field.shape[3]
        plan = plan_of(block_y * rows, rows, cols, block_x, block_y)
        if plan is None:
            return per_device(start_field, *rest)
        return fast_device(plan, start_field, *rest)

    return jax.shard_map(
        body,
        mesh=mesh,
        in_specs=(P(None, None, "col", "row"),) * 5,
        out_specs=P(None, None, "col", "row"),
        check_vma=False,
    )
```
